32 devices in a mesh: rep: 2 (over x), y: 4 (over z), x: 4 (over y, core).
Axes of the slice: x: 2, y: 2, z: 4, core: 2. Of those that a mesh axis runs over, the one named last changes fastest.
Arguments:
- hidden: bfloat16 [64, 4096], P('rep', 'y'), parts along dimension 0
- lengths: int32 [64], P('rep'), parts along dimension 0
- k_cache: bfloat16 [2, 64, 128, 32, 128], P(None, ('rep', 'y'), None, 'x'), parts along dimension 1
- v_cache: bfloat16 [2, 64, 128, 32, 128], P(None, ('rep', 'y'), None, 'x'), parts along dimension 1
- rel_table: bfloat16 [2, 128, 32, 128], P(None, None, 'x')
- norm_attn: bfloat16 [2, 4096], P(None, 'y')
- w_q: bfloat16 [2, 4096, 32, 128], P(None, 'y', 'x')
- w_k: bfloat16 [2, 4096, 32, 128], P(None, 'y', 'x')
- w_v: bfloat16 [2, 4096, 32, 128], P(None, 'y', 'x')
- bias_content: bfloat16 [2, 32, 128], P(None, 'x')
- bias_pos: bfloat16 [2, 32, 128], P(None, 'x')
- w_out: bfloat16 [2, 32, 128, 4096], P(None, 'x', None, 'y')
- norm_mlp: bfloat16 [2, 4096], P(None, 'y')
- w_up: bfloat16 [2, 4096, 16384], P(None, 'y', 'x')
- w_down: bfloat16 [2, 16384, 4096], P(None, 'x', 'y')
Outputs:
- output 1: bfloat16 [64, 4096], P('rep', 'y'), parts along dimension 0
- output 2: bfloat16 [2, 64, 128, 32, 128], P(None, ('rep', 'y'), None, 'x'), parts along dimension 1
- output 3: bfloat16 [2, 64, 128, 32, 128], P(None, ('rep', 'y'), None, 'x'), parts along dimension 1
There are 2 independent parts. The reference program is written for one: setup_inputs(seed, part) draws one part's arguments, and reference() takes and returns one part's arrays. A program takes and returns all parts, laid end to end along the dimension named above; an argument that names none is the same for every part.
All inputs are finite; a program needn't handle non-finite values.
Results may differ from the reference program's by a relative error of at most 0.0197235.
Values are sent between devices in bfloat16 or wider.
A program may use at most 1 GiB of HBM per device.

```python
import jax
import jax.numpy as jnp
from jax import lax

D_MODEL = 4096
HEADS = 32
HEAD_DIM = 128
FF_DIM = 16384
SEQ_MAX = 128
BATCH_ROWS = 32
LAYERS = 2

LEN_LOW = max(1, SEQ_MAX // 10)


def relative_table(key):
    feat_half = 64
    dist = jnp.arange(SEQ_MAX, dtype=jnp.float32)
    freqs = 10000.0 ** (-jnp.arange(feat_half, dtype=jnp.float32) / feat_half)
    angle = dist[:, None] * freqs[None, :]
    feats = jnp.concatenate([jnp.sin(angle), jnp.cos(angle)], axis=1)
    proj = jax.random.normal(key, (LAYERS, 2 * feat_half, HEADS * HEAD_DIM), jnp.float32) * feat_half ** -0.5
    table = jnp.einsum("tf,lfe->lte", feats, proj)
    return table.reshape(LAYERS, SEQ_MAX, HEADS, HEAD_DIM).astype(jnp.bfloat16)


def setup_inputs(seed: int = 0, part: int = 0) -> dict:
    base_key = jax.random.key(seed)
    shared = jax.random.split(base_key, 11)
    part_keys = jax.random.split(jax.random.fold_in(base_key, part), 4)

    def normal(key, shape, scale):
        return (jax.random.normal(key, shape, jnp.float32) * scale).astype(jnp.bfloat16)

    def gains(key):
        return (1.0 + 0.3 * jax.random.normal(key, (LAYERS, D_MODEL), jnp.float32)).astype(jnp.bfloat16)

    model_scale = D_MODEL ** -0.5
    out_scale = (HEADS * HEAD_DIM) ** -0.5 * (SEQ_MAX / 64) ** 0.5
    proj_shape = (LAYERS, D_MODEL, HEADS, HEAD_DIM)
    cache_shape = (LAYERS, BATCH_ROWS, SEQ_MAX, HEADS, HEAD_DIM)
    lengths = jax.random.randint(part_keys[3], (BATCH_ROWS,), LEN_LOW, SEQ_MAX, dtype=jnp.int32)
    lengths = lengths.at[0].set(SEQ_MAX - 1).at[1].set(LEN_LOW)
    return {
        "hidden": normal(part_keys[0], (BATCH_ROWS, D_MODEL), 1.0),
        "lengths": lengths,
        "k_cache": normal(part_keys[1], cache_shape, 1.0),
        "v_cache": normal(part_keys[2], cache_shape, 1.0),
        "rel_table": relative_table(shared[0]),
        "norm_attn": gains(shared[1]),
        "w_q": normal(shared[2], proj_shape, model_scale),
        "w_k": normal(shared[3], proj_shape, model_scale),
        "w_v": normal(shared[4], proj_shape, model_scale),
        "bias_content": normal(shared[5], (LAYERS, HEADS, HEAD_DIM), 0.5),
        "bias_pos": normal(shared[6], (LAYERS, HEADS, HEAD_DIM), 0.5),
        "w_out": normal(shared[7], (LAYERS, HEADS, HEAD_DIM, D_MODEL), out_scale),
        "norm_mlp": gains(shared[8]),
        "w_up": normal(shared[9], (LAYERS, D_MODEL, FF_DIM), model_scale),
        "w_down": normal(shared[10], (LAYERS, FF_DIM, D_MODEL), FF_DIM ** -0.5),
    }


def rms_norm(values, gain):
    wide = values.astype(jnp.float32)
    inv_rms = lax.rsqrt(jnp.mean(wide * wide, axis=-1, keepdims=True) + 1e-6)
    return (wide * inv_rms * gain.astype(jnp.float32)).astype(jnp.bfloat16)


def project(normed, weight):
    flat = jnp.dot(normed, weight.reshape(D_MODEL, HEADS * HEAD_DIM), preferred_element_type=jnp.float32)
    return flat.reshape(BATCH_ROWS, HEADS, HEAD_DIM).astype(jnp.bfloat16)


def reference(hidden, lengths, k_cache, v_cache, rel_table, norm_attn, w_q, w_k, w_v, bias_content, bias_pos, w_out, norm_mlp, w_up, w_down):
    positions = jnp.arange(SEQ_MAX)
    row_ids = jnp.arange(BATCH_ROWS)

    def layer_step(state, layer_args):
        (k_layer, v_layer, rel_layer, gain_attn, wq_layer, wk_layer, wv_layer,
         content_bias, pos_bias, wout_layer, gain_mlp, wup_layer, wdown_layer) = layer_args
        normed = rms_norm(state, gain_attn)
        q_new = project(normed, wq_layer)
        k_new = project(normed, wk_layer)
        v_new = project(normed, wv_layer)
        k_upd = k_layer.at[row_ids, lengths].set(k_new)
        v_upd = v_layer.at[row_ids, lengths].set(v_new)
        rel_wide = rel_layer.astype(jnp.float32)
        cbias_wide = content_bias.astype(jnp.float32)
        pbias_wide = pos_bias.astype(jnp.float32)

        def attend_row(row_args):
            q_row, k_rows, v_rows, length = row_args
            q_wide = q_row.astype(jnp.float32)
            q_content = (q_wide + cbias_wide).astype(jnp.bfloat16).astype(jnp.float32)
            q_pos = (q_wide + pbias_wide).astype(jnp.bfloat16).astype(jnp.float32)
            rel_rows = jnp.take(rel_wide, jnp.maximum(length - positions, 0), axis=0)
            scores = jnp.einsum("he,she->hs", q_content, k_rows.astype(jnp.float32))
            scores = scores + jnp.einsum("he,she->hs", q_pos, rel_rows)
            scores = jnp.where(positions[None, :] <= length, scores * HEAD_DIM ** -0.5, -1e30)
            attn_prob = jax.nn.softmax(scores, axis=-1).astype(jnp.bfloat16).astype(jnp.float32)
            return jnp.einsum("hs,she->he", attn_prob, v_rows.astype(jnp.float32)).astype(jnp.bfloat16)

        context = lax.map(attend_row, (q_new, k_upd, v_upd, lengths))
        attn_out = jnp.dot(context.reshape(BATCH_ROWS, HEADS * HEAD_DIM), wout_layer.reshape(HEADS * HEAD_DIM, D_MODEL), preferred_element_type=jnp.float32)
        state = (state.astype(jnp.float32) + attn_out).astype(jnp.bfloat16)
        normed = rms_norm(state, gain_mlp)
        up_proj = jnp.dot(normed, wup_layer, preferred_element_type=jnp.float32).astype(jnp.bfloat16)
        activated = jax.nn.gelu(up_proj.astype(jnp.float32), approximate=True).astype(jnp.bfloat16)
        down_out = jnp.dot(activated, wdown_layer, preferred_element_type=jnp.float32)
        state = (state.astype(jnp.float32) + down_out).astype(jnp.bfloat16)
        return state, (k_upd, v_upd)

    final, (k_all, v_all) = lax.scan(layer_step, hidden, (k_cache, v_cache, rel_table, norm_attn, w_q, w_k, w_v, bias_content, bias_pos, w_out, norm_mlp, w_up, w_down))
    return final, k_all, v_all
```

```python
import functools

import jax
import jax.numpy as jnp
from jax import lax
from jax.experimental import pallas as pl
from jax.experimental.pallas import tpu as pltpu
from jax.sharding import PartitionSpec as P

EPS = 1e-6
MESH = pl.DeviceIdType.MESH
BF16 = jnp.bfloat16
F32 = jnp.float32
NT = (((1,), (1,)), ((), ()))


def dot(a, b):
    return jnp.dot(a, b, preferred_element_type=F32)


def layers_kernel(
    ny, nx,
    x_ref, len_ref, k_hbm, v_hbm, rel_hbm, ga_ref, wq_hbm, wk_hbm, wv_hbm, u_ref, w_ref, wo_hbm, gm_ref, wup_hbm, wdn_hbm,
    xout_ref, knew_ref, vnew_ref,
    wq, wk, wv, wo, wup, wdn, kbuf, vbuf, rel, relrev,
    xcur, hs, expand, acc, qkv_send, qkv_recv, stat, qkvf, ctxf, ctx_recv, lhs_wo, ar, up_send, up_recv, act,
    wsem, send_sem, recv_sem,
):
    layers = wup_hbm.shape[0]
    rows, dm = x_ref.shape
    rloc = rows // ny
    heads, hd = u_ref.shape[1:]
    ffc = wup.shape[3]
    seq = rel_hbm.shape[1]
    nblk = dm // 128
    r = lax.axis_index("rep")
    y = lax.axis_index("y")
    x = lax.axis_index("x")

    def loads(l):
        out = [
            (wq_hbm.at[l], wq.at[l]), (wk_hbm.at[l], wk.at[l]), (wv_hbm.at[l], wv.at[l]),
            (k_hbm.at[l], kbuf.at[l]), (rel_hbm.at[l], rel.at[l]), (v_hbm.at[l], vbuf.at[l]), (wo_hbm.at[l], wo.at[l]),
        ]
        for c in range(ny):
            out.append((wup_hbm.at[l, :, pl.ds(c * ffc, ffc)], wup.at[l, c]))
        for c in range(ny):
            out.append((wdn_hbm.at[l, pl.ds(c * ffc, ffc), :], wdn.at[l, c]))
        return [pltpu.make_async_copy(s, d, wsem.at[l, i]) for i, (s, d) in enumerate(out)]

    for l in range(layers):
        for c in loads(l):
            c.start()

    barrier = pltpu.get_barrier_semaphore()
    for d in range(1, ny):
        pl.semaphore_signal(barrier, inc=1, device_id=(r, lax.rem(y + d, ny), x), device_id_type=MESH)
    for d in range(1, nx):
        pl.semaphore_signal(barrier, inc=1, device_id=(r, y, lax.rem(x + d, nx)), device_id_type=MESH)

    xcur[...] = x_ref[...]
    e_row = lax.broadcasted_iota(jnp.int32, (128, 128 * heads), 0)
    e_col = lax.broadcasted_iota(jnp.int32, (128, 128 * heads), 1)
    expand[...] = jnp.where(e_col // heads == e_row, 1.0, 0.0).astype(BF16)

    pl.semaphore_wait(barrier, (ny - 1) + (nx - 1))

    def send(l, ph, src, dst, device, to):
        me, peer = to
        return pltpu.make_async_remote_copy(
            src_ref=src, dst_ref=dst, send_sem=send_sem.at[l, ph, peer], recv_sem=recv_sem.at[l, ph, me],
            device_id=device, device_id_type=MESH)

    def recv_wait(l, ph, buf, frm):
        pltpu.make_async_remote_copy(
            src_ref=buf, dst_ref=buf, send_sem=send_sem.at[l, ph, frm], recv_sem=recv_sem.at[l, ph, frm],
            device_id=(r, y, x), device_id_type=MESH).wait_recv()

    def send_wait(l, ph, buf, to):
        pltpu.make_async_remote_copy(
            src_ref=buf, dst_ref=buf, send_sem=send_sem.at[l, ph, to], recv_sem=recv_sem.at[l, ph, to],
            device_id=(r, y, x), device_id_type=MESH).wait_send()

    i32 = lax.broadcasted_iota(jnp.int32, (rows, 128), 0)
    l32 = lax.broadcasted_iota(jnp.int32, (rows, 128), 1)
    i8 = lax.broadcasted_iota(jnp.int32, (8, 128), 0)
    l8 = lax.broadcasted_iota(jnp.int32, (8, 128), 1)

    def gain_row(ref, l):
        g = ref[...].astype(F32)
        row = g[0:1]
        for i in range(1, layers):
            row = jnp.where(l == i, g[i:i + 1], row)
        return row

    def norm_local(l, ph, gain):
        xw = xcur[...].astype(F32)
        t = jnp.sum(xw * xw, axis=1, keepdims=True) * (1.0 / dm) + EPS
        t_row = jnp.sum(jnp.where(i32 == l32, jnp.broadcast_to(t, (rows, 128)), 0.0), axis=0, keepdims=True)
        stat[l, ph, y] = jnp.broadcast_to(t_row, (8, 128))
        for d in range(1, ny):
            py = lax.rem(y + d, ny)
            send(l, ph, stat.at[l, ph, y], stat.at[l, ph, y], (r, py, x), (y, py)).start()
        return (xw * lax.rsqrt(t) * gain).astype(BF16)

    def ratio_rows(l, ph):
        for d in range(1, ny):
            py = lax.rem(y + d, ny)
            recv_wait(l, ph, stat.at[l, ph, py], py)
        ts = [stat[l, ph, p] for p in range(ny)]
        mean = ts[0]
        for p in range(1, ny):
            mean = mean + ts[p]
        inv = lax.rsqrt(mean * (1.0 / ny))
        return [jnp.sqrt(t) * inv for t in ts]

    def all_reduce_x(l, ph, slot):
        for d in range(1, nx):
            px = lax.rem(x + d, nx)
            send(l, ph, ar.at[l, slot, x], ar.at[l, slot, x], (r, y, px), (x, px)).start()
        for d in range(1, nx):
            px = lax.rem(x + d, nx)
            recv_wait(l, ph, ar.at[l, slot, px], px)
        total = ar[l, slot, 0].astype(F32)
        for p in range(1, nx):
            total = total + ar[l, slot, p].astype(F32)
        xcur[...] = (xcur[...].astype(F32) + total).astype(BF16)

    def layer(l, carry):
        w = loads(l)
        h = norm_local(l, 0, gain_row(ga_ref, l))
        for b in range(nblk):
            hs[b] = h[:, b * 128:(b + 1) * 128]
        acc[...] = jnp.zeros_like(acc)
        w[0].wait()
        w[1].wait()
        w[2].wait()
        lane = lax.broadcasted_iota(jnp.int32, (rows, 128 * heads), 1) % heads

        def qkv_block(b, c):
            hx = dot(hs[b], expand[...])
            lhs = jnp.concatenate([jnp.where(lane == j, hx, 0.0) for j in range(heads)], axis=0).astype(BF16)
            ks = pl.ds(pl.multiple_of(b * 128 * heads, 128 * heads), 128 * heads)
            for i, wt in enumerate((wq, wk, wv)):
                acc[i] += dot(lhs, wt[l, ks, :])
            return c

        lax.fori_loop(0, nblk, qkv_block, 0)
        for p in range(ny):
            for i in range(3):
                a3 = acc[i].reshape(heads, rows, hd)
                qkv_send[p, i * heads:(i + 1) * heads] = a3[:, p * rloc:(p + 1) * rloc, :].astype(BF16)
        for d in range(1, ny):
            py = lax.rem(y + d, ny)
            send(l, 1, qkv_send.at[py], qkv_recv.at[l, y], (r, py, x), (y, py)).start()
        qkv_recv[l, y] = qkv_send[y]

        w[4].wait()

        def rev(t, c):
            relrev[seq - 1 - t] = rel[l, t]
            return c

        lax.fori_loop(0, seq, rev, 0)
        relrev[pl.ds(seq, seq)] = jnp.zeros((seq, heads, hd), BF16)

        ratios = ratio_rows(l, 0)
        cols = [jnp.sum(jnp.where(l8 == i8 + rloc * y, ra, 0.0), axis=1, keepdims=True) for ra in ratios]
        for d in range(1, ny):
            py = lax.rem(y + d, ny)
            recv_wait(l, 1, qkv_recv.at[l, py], py)
        tot = qkv_recv[l, 0].astype(F32) * cols[0][None]
        for p in range(1, ny):
            tot = tot + qkv_recv[l, p].astype(F32) * cols[p][None]
        qkvf[...] = tot.astype(BF16).astype(F32).reshape(3 * heads * rloc, hd)

        w[3].wait()
        w[5].wait()
        ul = u_ref[l].astype(F32)
        wl = w_ref[l].astype(F32)
        rel0 = relrev[seq - 1].astype(F32)
        sub = lax.broadcasted_iota(jnp.int32, (heads, seq * heads), 0)
        col = lax.broadcasted_iota(jnp.int32, (heads, seq * heads), 1)
        own = (col % heads) == sub
        pos = col // heads
        scale = hd ** -0.5

        def attend(b, c):
            length = len_ref[rloc * y + b]
            q = qkvf[pl.ds(b, heads, stride=rloc), :]
            k = qkvf[pl.ds(heads * rloc + b, heads, stride=rloc), :]
            v = qkvf[pl.ds(2 * heads * rloc + b, heads, stride=rloc), :]
            knew_ref[l, b] = k.astype(BF16)
            vnew_ref[l, b] = v.astype(BF16)
            a = (q + ul).astype(BF16)
            cc = (q + wl).astype(BF16)
            window = relrev[pl.ds(seq - 1 - length, seq)].reshape(seq * heads, hd)
            s = lax.dot_general(a, kbuf[l, b], NT, preferred_element_type=F32)
            s = s + lax.dot_general(cc, window, NT, preferred_element_type=F32)
            s = jnp.where(own & (pos < length), s * scale, -1e30)
            sn = jnp.sum(a.astype(F32) * k + cc.astype(F32) * rel0, axis=1, keepdims=True) * scale
            m = jnp.maximum(jnp.max(s, axis=1, keepdims=True), sn)
            e = jnp.exp(s - m)
            en = jnp.exp(sn - m)
            z = jnp.sum(e, axis=1, keepdims=True) + en
            pr = (e / z).astype(BF16)
            pn = (en / z).astype(BF16).astype(F32)
            ctx = dot(pr, vbuf[l, b]) + pn * v
            ctxf[pl.ds(pl.multiple_of(b * heads, heads), heads), :] = ctx
            return c

        for b in range(rloc):
            attend(b, 0)
        for j in range(heads):
            ctx_recv[l, y, j] = ctxf[pl.ds(j, rloc, stride=heads), :].astype(BF16)
        for d in range(1, ny):
            py = lax.rem(y + d, ny)
            send(l, 2, ctx_recv.at[l, y], ctx_recv.at[l, y], (r, py, x), (y, py)).start()
        for d in range(1, ny):
            py = lax.rem(y + d, ny)
            recv_wait(l, 2, ctx_recv.at[l, py], py)

        for j in range(heads):
            lhs_wo[:, j * hd:(j + 1) * hd] = jnp.concatenate(
                [ctx_recv[l, p, j].astype(F32) for p in range(ny)], axis=0).astype(BF16)
        w[6].wait()
        ar[l, 0, x] = dot(lhs_wo[...], wo[l]).astype(BF16)
        all_reduce_x(l, 3, 0)

        h2 = norm_local(l, 4, gain_row(gm_ref, l))
        for i in range(ny):
            w[7 + i].wait()
        hs_flat = h2

        for d in range(1, ny + 1):
            py = lax.rem(y + d, ny)
            part = dot(hs_flat, wup[l, py]).astype(BF16)
            if d < ny:
                up_send[py] = part
                send(l, 5, up_send.at[py], up_recv.at[l, y], (r, py, x), (y, py)).start()
            else:
                up_recv[l, y] = part
        ratios = ratio_rows(l, 4)
        cols = [jnp.sum(jnp.where(l32 == i32, ra[0:1], 0.0), axis=1, keepdims=True) for ra in ratios]
        for d in range(1, ny):
            py = lax.rem(y + d, ny)
            recv_wait(l, 5, up_recv.at[l, py], py)
        up = up_recv[l, 0].astype(F32) * cols[0]
        for p in range(1, ny):
            up = up + up_recv[l, p].astype(F32) * cols[p]
        up = up.astype(BF16).astype(F32)
        act[l, y] = jax.nn.gelu(up, approximate=True).astype(BF16)
        for d in range(1, ny):
            py = lax.rem(y + d, ny)
            send(l, 6, act.at[l, y], act.at[l, y], (r, py, x), (y, py)).start()
        for i in range(ny):
            w[7 + ny + i].wait()
        down = dot(act[l, y], wdn[l, y])
        for d in range(1, ny):
            py = lax.rem(y + d, ny)
            recv_wait(l, 6, act.at[l, py], py)
            down = down + dot(act[l, py], wdn[l, py])
        ar[l, 1, x] = down.astype(BF16)
        all_reduce_x(l, 7, 1)
        for d in range(1, ny):
            py = lax.rem(y + d, ny)
            send_wait(l, 1, qkv_send.at[py], py)
            send_wait(l, 5, up_send.at[py], py)
        return carry

    lax.fori_loop(0, layers, layer, 0)
    xout_ref[...] = xcur[...]

    def drain(l, carry):
        for d in range(1, ny):
            py = lax.rem(y + d, ny)
            send_wait(l, 0, stat.at[l, 0, y], py)
            send_wait(l, 2, ctx_recv.at[l, y], py)
            send_wait(l, 4, stat.at[l, 4, y], py)
            send_wait(l, 6, act.at[l, y], py)
        for d in range(1, nx):
            px = lax.rem(x + d, nx)
            send_wait(l, 3, ar.at[l, 0, x], px)
            send_wait(l, 7, ar.at[l, 1, x], px)
        return carry

    lax.fori_loop(0, layers, drain, 0)


def write_rows(cache, new_rows, lengths):
    hit = jnp.arange(cache.shape[2])[None, None, :] == lengths[None, :, None]
    return jnp.where(hit[:, :, :, None, None], new_rows[:, :, None, :, :], cache)


def solution(mesh):
    ny, nx = mesh.shape["y"], mesh.shape["x"]
    cache_spec = P(None, ("rep", "y"), None, "x", None)
    row_spec = P("rep", "y")
    proj_spec = P(None, "y", "x", None)
    head_spec = P(None, "x", None)
    in_specs = (row_spec, P("rep"), cache_spec, cache_spec, P(None, None, "x", None), P(None, "y"),
                proj_spec, proj_spec, proj_spec, head_spec, head_spec, P(None, "x", None, "y"),
                P(None, "y"), P(None, "y", "x"), P(None, "x", "y"))
    out_specs = (row_spec, cache_spec, cache_spec)

    def local_step(hidden, lengths, k_cache, v_cache, rel_table, norm_attn, w_q, w_k, w_v, bias_content, bias_pos, w_out, norm_mlp, w_up, w_down):
        rows, dm = hidden.shape
        layers, rloc, seq, heads, hd = k_cache.shape
        ff = w_up.shape[2]
        ffc = ff // ny
        flat = (layers, dm * heads, hd)
        vm = pl.BlockSpec(memory_space=pltpu.VMEM)
        sm = pl.BlockSpec(memory_space=pltpu.SMEM)
        hbm = pl.BlockSpec(memory_space=pl.ANY)
        new_shape = jax.ShapeDtypeStruct((layers, rloc, heads, hd), BF16)
        nph = 8
        npeer = max(ny, nx)
        out, k_new, v_new = pl.pallas_call(
            functools.partial(layers_kernel, ny, nx),
            name="decode_layers",
            out_shape=(jax.ShapeDtypeStruct((rows, dm), BF16), new_shape, new_shape),
            in_specs=[vm, sm, hbm, hbm, hbm, vm, hbm, hbm, hbm, vm, vm, hbm, vm, hbm, hbm],
            out_specs=(vm, vm, vm),
            scratch_shapes=[
                pltpu.VMEM(flat, BF16), pltpu.VMEM(flat, BF16), pltpu.VMEM(flat, BF16),
                pltpu.VMEM((layers, heads * hd, dm), BF16),
                pltpu.VMEM((layers, ny, dm, ffc), BF16),
                pltpu.VMEM((layers, ny, ffc, dm), BF16),
                pltpu.VMEM((layers, rloc, seq * heads, hd), BF16),
                pltpu.VMEM((layers, rloc, seq * heads, hd), BF16),
                pltpu.VMEM((layers, seq, heads, hd), BF16),
                pltpu.VMEM((2 * seq, heads, hd), BF16),
                pltpu.VMEM((rows, dm), BF16),
                pltpu.VMEM((dm // 128, rows, 128), BF16),
                pltpu.VMEM((128, 128 * heads), BF16),
                pltpu.VMEM((3, heads * rows, hd), F32),
                pltpu.VMEM((ny, 3 * heads, rloc, hd), BF16),
                pltpu.VMEM((layers, ny, 3 * heads, rloc, hd), BF16),
                pltpu.VMEM((layers, nph, ny, 8, 128), F32),
                pltpu.VMEM((3 * heads * rloc, hd), F32),
                pltpu.VMEM((rloc * heads, hd), F32),
                pltpu.VMEM((layers, ny, heads, rloc, hd), BF16),
                pltpu.VMEM((rows, heads * hd), BF16),
                pltpu.VMEM((layers, 2, nx, rows, dm), BF16),
                pltpu.VMEM((ny, rows, ffc), BF16),
                pltpu.VMEM((layers, ny, rows, ffc), BF16),
                pltpu.VMEM((layers, ny, rows, ffc), BF16),
                pltpu.SemaphoreType.DMA((layers, 7 + 2 * ny)),
                pltpu.SemaphoreType.DMA((layers, nph, npeer)),
                pltpu.SemaphoreType.DMA((layers, nph, npeer)),
            ],
            compiler_params=pltpu.CompilerParams(
                collective_id=0, has_side_effects=True, vmem_limit_bytes=67043328),
        )(hidden, lengths, k_cache.reshape(layers, rloc, seq * heads, hd), v_cache.reshape(layers, rloc, seq * heads, hd),
          rel_table, norm_attn, w_q.reshape(flat), w_k.reshape(flat), w_v.reshape(flat), bias_content, bias_pos,
          w_out.reshape(layers, heads * hd, dm), norm_mlp, w_up, w_down)
        row_start = lax.axis_index("y") * rloc
        len_local = lax.dynamic_slice_in_dim(lengths, row_start, rloc)
        return out, write_rows(k_cache, k_new, len_local), write_rows(v_cache, v_new, len_local)

    return jax.shard_map(local_step, mesh=mesh, in_specs=in_specs, out_specs=out_specs, check_vma=False)
```

```python
import functools

import jax
import jax.numpy as jnp
from jax import lax
from jax.experimental import pallas as pl
from jax.experimental.pallas import tpu as pltpu
from jax.sharding import PartitionSpec as P

EPS = 1e-6
MESH = pl.DeviceIdType.MESH
BF16 = jnp.bfloat16
F32 = jnp.float32
NT = (((1,), (1,)), ((), ()))


def dot(a, b):
    return jnp.dot(a, b, preferred_element_type=F32)


def layers_kernel(
    ny, nx, nch,
    x_ref, len_ref, k_hbm, v_hbm, rel_hbm, ga_ref, wq_hbm, wk_hbm, wv_hbm, u_ref, w_ref, wo_hbm, gm_ref, wup_hbm, wdn_hbm,
    xout_ref, knew_ref, vnew_ref,
    wq, wk, wv, wo, wup, wdn, kbuf, vbuf, rel, relrev,
    xcur, hs, expand, lhs, qkv_send, qkv_recv, stat, qkvf, scores, ctxf, ctx_recv, lhs_wo, ar, up_send, up_recv, act, down,
    wsem, send_sem, recv_sem,
):
    layers = wup_hbm.shape[0]
    rows, dm = x_ref.shape
    rloc = rows // ny
    heads, hd = u_ref.shape[1:]
    ffc = wup.shape[3]
    sub_ff = ffc // nch
    seq = rel_hbm.shape[1]
    nblk = dm // 128
    wide = 128 * heads
    r = lax.axis_index("rep")
    y = lax.axis_index("y")
    x = lax.axis_index("x")
    half = y // 2
    ypeers = [3 - 3 * half, 2 - half, 1 - y + 4 * half] if ny == 4 else [lax.rem(y + d, ny) for d in range(1, ny)]
    xpeers = [lax.rem(x + 2, nx), 3 - x, x + 1 - 2 * lax.rem(x, 2)] if nx == 4 else [lax.rem(x + d, nx) for d in range(1, nx)]

    def load_qkv(l):
        pairs = [(wq_hbm.at[l], wq), (wk_hbm.at[l], wk), (wv_hbm.at[l], wv)]
        return [pltpu.make_async_copy(s, d, wsem.at[l, i]) for i, (s, d) in enumerate(pairs)]

    def load_rest(l):
        out = [(k_hbm.at[l], kbuf.at[l]), (rel_hbm.at[l], rel.at[l]), (v_hbm.at[l], vbuf.at[l]), (wo_hbm.at[l], wo.at[l])]
        for c in range(ny):
            out.append((wup_hbm.at[l, :, pl.ds(c * ffc, ffc)], wup.at[l, c]))
        for c in range(ny):
            out.append((wdn_hbm.at[l, pl.ds(c * ffc, ffc), :], wdn.at[l, c]))
        return [pltpu.make_async_copy(s, d, wsem.at[l, 3 + i]) for i, (s, d) in enumerate(out)]

    for c in load_qkv(0):
        c.start()
    for l in range(layers):
        for c in load_rest(l):
            c.start()

    barrier = pltpu.get_barrier_semaphore()
    for py in ypeers:
        pl.semaphore_signal(barrier, inc=1, device_id=(r, py, x), device_id_type=MESH)
    for px in xpeers:
        pl.semaphore_signal(barrier, inc=1, device_id=(r, y, px), device_id_type=MESH)

    xcur[...] = x_ref[...]
    e_row = lax.broadcasted_iota(jnp.int32, (128, wide), 0)
    e_col = lax.broadcasted_iota(jnp.int32, (128, wide), 1)
    expand[...] = jnp.where(e_col // heads == e_row, 1.0, 0.0).astype(BF16)
    i32 = lax.broadcasted_iota(jnp.int32, (rows, 128), 0)
    l32 = lax.broadcasted_iota(jnp.int32, (rows, 128), 1)
    i8 = lax.broadcasted_iota(jnp.int32, (8, 128), 0)
    l8 = lax.broadcasted_iota(jnp.int32, (8, 128), 1)

    pl.semaphore_wait(barrier, (ny - 1) + (nx - 1))

    def copy_y(l, ph, src, dst, py):
        return pltpu.make_async_remote_copy(
            src_ref=src, dst_ref=dst, send_sem=send_sem.at[l, ph, py], recv_sem=recv_sem.at[l, ph, y],
            device_id=(r, py, x), device_id_type=MESH)

    def copy_x(l, ph, src, dst, px):
        return pltpu.make_async_remote_copy(
            src_ref=src, dst_ref=dst, send_sem=send_sem.at[l, ph, px], recv_sem=recv_sem.at[l, ph, x],
            device_id=(r, y, px), device_id_type=MESH)

    def local(l, ph, buf, i):
        return pltpu.make_async_remote_copy(
            src_ref=buf, dst_ref=buf, send_sem=send_sem.at[l, ph, i], recv_sem=recv_sem.at[l, ph, i],
            device_id=(r, y, x), device_id_type=MESH)

    def gain_row(ref, l):
        g = ref[...].astype(F32)
        row = g[0:1]
        for i in range(1, layers):
            row = jnp.where(l == i, g[i:i + 1], row)
        return row

    def norm_local(l, ph, gain):
        xw = xcur[...].astype(F32)
        t = jnp.sum(xw * xw, axis=1, keepdims=True) * (1.0 / dm) + EPS
        t_row = jnp.sum(jnp.where(i32 == l32, jnp.broadcast_to(t, (rows, 128)), 0.0), axis=0, keepdims=True)
        stat[l, ph, y] = jnp.broadcast_to(t_row, (8, 128))
        for py in ypeers:
            copy_y(l, ph, stat.at[l, ph, y], stat.at[l, ph, y], py).start()
        return (xw * lax.rsqrt(t) * gain).astype(BF16)

    def ratio_rows(l, ph):
        for py in ypeers:
            local(l, ph, stat.at[l, ph, py], py).wait_recv()
        ts = [stat[l, ph, p] for p in range(ny)]
        mean = ts[0]
        for p in range(1, ny):
            mean = mean + ts[p]
        inv = lax.rsqrt(mean * (1.0 / ny))
        return [jnp.sqrt(t) * inv for t in ts]

    def all_reduce_x(l, ph, slot):
        for px in xpeers:
            copy_x(l, ph, ar.at[l, slot, x], ar.at[l, slot, x], px).start()
        for px in xpeers:
            local(l, ph, ar.at[l, slot, px], px).wait_recv()
        total = ar[l, slot, 0].astype(F32)
        for p in range(1, nx):
            total = total + ar[l, slot, p].astype(F32)
        xcur[...] = (xcur[...].astype(F32) + total).astype(BF16)

    PQ, PC, PA, PD, PU, PG = 2, 5, 6, 7, 8, 8 + nch

    def layer(l, carry):
        wl_qkv = load_qkv(l)
        wl = load_rest(l)
        h = norm_local(l, 0, gain_row(ga_ref, l))
        for b in range(nblk):
            hs[b * rows:(b + 1) * rows, :] = h[:, b * 128:(b + 1) * 128]
        lane = lax.broadcasted_iota(jnp.int32, (rows, wide), 1) % heads
        for b in range(nblk):
            hx = dot(hs[b * rows:(b + 1) * rows, :], expand[...])
            if b >= nblk // 2:
                hx = -hx
            for j in range(heads):
                lhs[j * rows:(j + 1) * rows, b * wide:(b + 1) * wide] = jnp.where(lane == j, hx, 0.0).astype(BF16)

        def scatter(i, part):
            a3 = part.reshape(heads, rows, hd)
            for p in range(ny):
                qkv_send[i, p] = a3[:, p * rloc:(p + 1) * rloc, :].astype(BF16)
            for py in ypeers:
                copy_y(l, PQ + i, qkv_send.at[i, py], qkv_recv.at[l, i, y], py).start()
            qkv_recv[l, i, y] = qkv_send[i, y]

        wl_qkv[0].wait()
        wl_qkv[1].wait()
        kh = dm * heads // 2
        qk = (dot(lhs[:, :kh], jnp.concatenate([wq[:kh, :], wk[:kh, :]], axis=1))
              - dot(lhs[:, kh:], jnp.concatenate([wq[kh:, :], wk[kh:, :]], axis=1)))
        scatter(0, qk[:, :hd])
        scatter(1, qk[:, hd:])
        wl_qkv[2].wait()
        scatter(2, dot(lhs[:, :kh], wv[:kh, :]) - dot(lhs[:, kh:], wv[kh:, :]))

        @pl.when(l + 1 < layers)
        def _():
            for c in load_qkv(l + 1):
                c.start()

        wl[1].wait()

        def rev(t, c):
            relrev[seq - 1 - t] = rel[l, t]
            return c

        lax.fori_loop(0, seq, rev, 0, unroll=8)
        relrev[pl.ds(seq, seq)] = jnp.zeros((seq, heads, hd), BF16)

        ratios = ratio_rows(l, 0)
        cols = [jnp.sum(jnp.where(l8 == i8 + rloc * y, ra, 0.0), axis=1, keepdims=True) for ra in ratios]

        def gather(i):
            for py in ypeers:
                local(l, PQ + i, qkv_recv.at[l, i, py], py).wait_recv()
            tot = qkv_recv[l, i, 0].astype(F32) * cols[0][None]
            for p in range(1, ny):
                tot = tot + qkv_recv[l, i, p].astype(F32) * cols[p][None]
            qkvf[i] = tot.astype(BF16).astype(F32).reshape(heads * rloc, hd)

        wl[0].wait()
        gather(0)
        ul = u_ref[l].astype(F32)
        wl_pos = w_ref[l].astype(F32)
        rel0 = relrev[seq - 1].astype(F32)
        sub = lax.broadcasted_iota(jnp.int32, (heads, seq * heads), 0)
        col = lax.broadcasted_iota(jnp.int32, (heads, seq * heads), 1)
        own = (col % heads) == sub
        pos = col // heads
        scale = hd ** -0.5

        def query(b):
            q = qkvf[0, pl.ds(b, heads, stride=rloc), :]
            return (q + ul).astype(BF16), (q + wl_pos).astype(BF16)

        for b in range(rloc):
            length = len_ref[rloc * y + b]
            a, cc = query(b)
            window = relrev[pl.ds(seq - 1 - length, seq)].reshape(seq * heads, hd)
            s = lax.dot_general(a, kbuf[l, b], NT, preferred_element_type=F32)
            s = s + lax.dot_general(cc, window, NT, preferred_element_type=F32)
            scores[b] = jnp.where(own & (pos < length), s * scale, -1e30)
        gather(1)
        wl[2].wait()
        gather(2)
        for b in range(rloc):
            a, cc = query(b)
            k = qkvf[1, pl.ds(b, heads, stride=rloc), :]
            v = qkvf[2, pl.ds(b, heads, stride=rloc), :]
            knew_ref[l, b] = k.astype(BF16)
            vnew_ref[l, b] = v.astype(BF16)
            s = scores[b]
            sn = jnp.sum(a.astype(F32) * k + cc.astype(F32) * rel0, axis=1, keepdims=True) * scale
            m = jnp.maximum(jnp.max(s, axis=1, keepdims=True), sn)
            e = jnp.exp(s - m)
            en = jnp.exp(sn - m)
            z = jnp.sum(e, axis=1, keepdims=True) + en
            pr = (e / z).astype(BF16)
            pn = (en / z).astype(BF16).astype(F32)
            ctxf[b * heads:(b + 1) * heads, :] = dot(pr, vbuf[l, b]) + pn * v
        for j in range(heads):
            ctx_recv[l, y, j] = ctxf[pl.ds(j, rloc, stride=heads), :].astype(BF16)
        for py in ypeers:
            copy_y(l, PC, ctx_recv.at[l, y], ctx_recv.at[l, y], py).start()
        for py in ypeers:
            local(l, PC, ctx_recv.at[l, py], py).wait_recv()

        for j in range(heads):
            lhs_wo[:, j * hd:(j + 1) * hd] = jnp.concatenate(
                [ctx_recv[l, p, j].astype(F32) for p in range(ny)], axis=0).astype(BF16)
        wl[3].wait()
        ar[l, 0, x] = dot(lhs_wo[...], wo[l]).astype(BF16)
        all_reduce_x(l, PA, 0)

        h2 = norm_local(l, 1, gain_row(gm_ref, l))
        for i in range(ny):
            wl[4 + i].wait()
        for ch in range(nch):
            cs = slice(ch * sub_ff, (ch + 1) * sub_ff)
            for py in ypeers:
                up_send[py, ch] = dot(h2, wup[l, py, :, cs]).astype(BF16)
                copy_y(l, PU + ch, up_send.at[py, ch], up_recv.at[l, y, ch], py).start()
            up_recv[l, y, ch] = dot(h2, wup[l, y, :, cs]).astype(BF16)
        ratios = ratio_rows(l, 1)
        cols2 = [jnp.sum(jnp.where(l32 == i32, ra[0:1], 0.0), axis=1, keepdims=True) for ra in ratios]
        for i in range(ny):
            wl[4 + ny + i].wait()
        for ch in range(nch):
            for py in ypeers:
                local(l, PU + ch, up_recv.at[l, py, ch], py).wait_recv()
            up = up_recv[l, 0, ch].astype(F32) * cols2[0]
            for p in range(1, ny):
                up = up + up_recv[l, p, ch].astype(F32) * cols2[p]
            up = up.astype(BF16).astype(F32)
            act[l, y, ch] = jax.nn.gelu(up, approximate=True).astype(BF16)
            for py in ypeers:
                copy_y(l, PG + ch, act.at[l, y, ch], act.at[l, y, ch], py).start()
            part = dot(act[l, y, ch], wdn[l, y, ch * sub_ff:(ch + 1) * sub_ff, :])
            if ch == 0:
                down[...] = part
            else:
                down[...] += part
        for ch in range(nch):
            for py in ypeers[::-1]:
                local(l, PG + ch, act.at[l, py, ch], py).wait_recv()
                down[...] += dot(act[l, py, ch], wdn[l, py, ch * sub_ff:(ch + 1) * sub_ff, :])
        ar[l, 1, x] = down[...].astype(BF16)
        all_reduce_x(l, PD, 1)
        for py in ypeers:
            for i in range(3):
                local(l, PQ + i, qkv_send.at[i, py], py).wait_send()
            for ch in range(nch):
                local(l, PU + ch, up_send.at[py, ch], py).wait_send()
        return carry

    lax.fori_loop(0, layers, layer, 0)
    xout_ref[...] = xcur[...]

    def drain(l, carry):
        for py in ypeers:
            local(l, 0, stat.at[l, 0, y], py).wait_send()
            local(l, 1, stat.at[l, 1, y], py).wait_send()
            local(l, PC, ctx_recv.at[l, y], py).wait_send()
            for ch in range(nch):
                local(l, PG + ch, act.at[l, y, ch], py).wait_send()
        for px in xpeers:
            local(l, PA, ar.at[l, 0, x], px).wait_send()
            local(l, PD, ar.at[l, 1, x], px).wait_send()
        return carry

    lax.fori_loop(0, layers, drain, 0)


def write_kernel(x_ref, len_ref, kn_ref, vn_ref, k_hbm, v_hbm, xout_ref, kout, vout, buf, in_sem, out_sem):
    layers, rloc = kn_ref.shape[:2]
    y = lax.axis_index("y")
    units = [(s, n, o, l) for l in range(layers) for s, n, o in ((k_hbm, kn_ref, kout), (v_hbm, vn_ref, vout))]
    nsplit = 2
    per = rloc // nsplit
    steps = [(s, n, o, l, q) for (s, n, o, l) in units for q in range(nsplit)]
    ins = [pltpu.make_async_copy(s.at[l, q * per:(q + 1) * per], buf.at[i], in_sem.at[i]) for i, (s, n, o, l, q) in enumerate(steps)]
    outs = [pltpu.make_async_copy(buf.at[i], o.at[l, q * per:(q + 1) * per], out_sem.at[i]) for i, (s, n, o, l, q) in enumerate(steps)]
    for c in ins:
        c.start()
    xout_ref[...] = x_ref[...]
    for i, (s, n, o, l, q) in enumerate(steps):
        ins[i].wait()
        for b in range(per):
            buf[i, b, len_ref[rloc * y + q * per + b]] = n[l, q * per + b]
        outs[i].start()
    for c in outs:
        c.wait()


def solution(mesh):
    ny, nx = mesh.shape["y"], mesh.shape["x"]
    cache_spec = P(None, ("rep", "y"), None, "x", None)
    row_spec = P("rep", "y")
    proj_spec = P(None, "y", "x", None)
    head_spec = P(None, "x", None)
    in_specs = (row_spec, P("rep"), cache_spec, cache_spec, P(None, None, "x", None), P(None, "y"),
                proj_spec, proj_spec, proj_spec, head_spec, head_spec, P(None, "x", None, "y"),
                P(None, "y"), P(None, "y", "x"), P(None, "x", "y"))
    out_specs = (row_spec, cache_spec, cache_spec)

    def local_step(hidden, lengths, k_cache, v_cache, rel_table, norm_attn, w_q, w_k, w_v, bias_content, bias_pos, w_out, norm_mlp, w_up, w_down):
        rows, dm = hidden.shape
        layers, rloc, seq, heads, hd = k_cache.shape
        ff = w_up.shape[2]
        ffc = ff // ny
        flat = (layers, dm * heads, hd)
        vm = pl.BlockSpec(memory_space=pltpu.VMEM)
        sm = pl.BlockSpec(memory_space=pltpu.SMEM)
        hbm = pl.BlockSpec(memory_space=pl.ANY)
        new_shape = jax.ShapeDtypeStruct((layers, rloc, heads, hd), BF16)
        nch = 2
        sub_ff = ffc // nch
        nph = 8 + 2 * nch
        npeer = max(ny, nx)
        out, k_new, v_new = pl.pallas_call(
            functools.partial(layers_kernel, ny, nx, nch),
            name="decode_layers",
            out_shape=(jax.ShapeDtypeStruct((rows, dm), BF16), new_shape, new_shape),
            in_specs=[vm, sm, hbm, hbm, hbm, vm, hbm, hbm, hbm, vm, vm, hbm, vm, hbm, hbm],
            out_specs=(vm, vm, vm),
            scratch_shapes=[
                pltpu.VMEM(flat[1:], BF16), pltpu.VMEM(flat[1:], BF16), pltpu.VMEM(flat[1:], BF16),
                pltpu.VMEM((layers, heads * hd, dm), BF16),
                pltpu.VMEM((layers, ny, dm, ffc), BF16),
                pltpu.VMEM((layers, ny, ffc, dm), BF16),
                pltpu.VMEM((layers, rloc, seq * heads, hd), BF16),
                pltpu.VMEM((layers, rloc, seq * heads, hd), BF16),
                pltpu.VMEM((layers, seq, heads, hd), BF16),
                pltpu.VMEM((2 * seq, heads, hd), BF16),
                pltpu.VMEM((rows, dm), BF16),
                pltpu.VMEM((dm // 128 * rows, 128), BF16),
                pltpu.VMEM((128, 128 * heads), BF16),
                pltpu.VMEM((heads * rows, dm * heads), BF16),
                pltpu.VMEM((3, ny, heads, rloc, hd), BF16),
                pltpu.VMEM((layers, 3, ny, heads, rloc, hd), BF16),
                pltpu.VMEM((layers, 2, ny, 8, 128), F32),
                pltpu.VMEM((3, heads * rloc, hd), F32),
                pltpu.VMEM((rloc, heads, seq * heads), F32),
                pltpu.VMEM((rloc * heads, hd), F32),
                pltpu.VMEM((layers, ny, heads, rloc, hd), BF16),
                pltpu.VMEM((rows, heads * hd), BF16),
                pltpu.VMEM((layers, 2, nx, rows, dm), BF16),
                pltpu.VMEM((ny, nch, rows, sub_ff), BF16),
                pltpu.VMEM((layers, ny, nch, rows, sub_ff), BF16),
                pltpu.VMEM((layers, ny, nch, rows, sub_ff), BF16),
                pltpu.VMEM((rows, dm), F32),
                pltpu.SemaphoreType.DMA((layers, 7 + 2 * ny)),
                pltpu.SemaphoreType.DMA((layers, nph, npeer)),
                pltpu.SemaphoreType.DMA((layers, nph, npeer)),
            ],
            compiler_params=pltpu.CompilerParams(
                collective_id=0, has_side_effects=True, vmem_limit_bytes=67043328),
        )(hidden, lengths, k_cache.reshape(layers, rloc, seq * heads, hd), v_cache.reshape(layers, rloc, seq * heads, hd),
          rel_table, norm_attn, w_q.reshape(flat), w_k.reshape(flat), w_v.reshape(flat), bias_content, bias_pos,
          w_out.reshape(layers, heads * hd, dm), norm_mlp, w_up, w_down)
        nunit = 2 * layers * 2
        cache_shape = jax.ShapeDtypeStruct(k_cache.shape, BF16)
        return pl.pallas_call(
            write_kernel,
            name="write_caches",
            out_shape=(jax.ShapeDtypeStruct((rows, dm), BF16), cache_shape, cache_shape),
            in_specs=[vm, sm, vm, vm, hbm, hbm],
            out_specs=(vm, hbm, hbm),
            scratch_shapes=[
                pltpu.VMEM((nunit, rloc // 2, seq, heads, hd), BF16),
                pltpu.SemaphoreType.DMA((nunit,)),
                pltpu.SemaphoreType.DMA((nunit,)),
            ],
            compiler_params=pltpu.CompilerParams(vmem_limit_bytes=16 << 20),
        )(out, lengths, k_new, v_new, k_cache, v_cache)

    return jax.shard_map(local_step, mesh=mesh, in_specs=in_specs, out_specs=out_specs, check_vma=False)
```

```python
import functools

import jax
import jax.numpy as jnp
from jax import lax
from jax.experimental import pallas as pl
from jax.experimental.pallas import tpu as pltpu
from jax.sharding import PartitionSpec as P

EPS = 1e-6
MESH = pl.DeviceIdType.MESH
BF16 = jnp.bfloat16
F32 = jnp.float32
NT = (((1,), (1,)), ((), ()))


def dot(a, b):
    return jnp.dot(a, b, preferred_element_type=F32)


def layers_kernel(
    ny, nx, ns,
    x_ref, len_ref, k_hbm, v_hbm, rel_hbm, ga_ref, wq_hbm, wk_hbm, wv_hbm, u_ref, w_ref, wo_hbm, gm_ref, wup_hbm, wdn_hbm,
    xout_ref, knew_ref, vnew_ref,
    wq, wk, wv, wo, wup, wdn, kbuf, vbuf, rel, relrev,
    xcur, hrep, expand, lhs, qkv_send, qkv_recv, stat, qkvf, ctxf, ctx_recv, lhs_wo, ar, up_send, up_recv, act, down,
    wsem, send_sem, recv_sem,
):
    layers = wup_hbm.shape[0]
    rows, dm = x_ref.shape
    rloc = rows // ny
    srow = rows // ns
    sloc = rloc // ns
    heads, hd = u_ref.shape[1:]
    ffc = wup.shape[3]
    seq = rel_hbm.shape[1]
    nblk = dm // 128
    wide = 128 * heads
    grp = heads * sloc
    r = lax.axis_index("rep")
    y = lax.axis_index("y")
    x = lax.axis_index("x")
    half = y // 2
    ypeers = [3 - 3 * half, 2 - half, 1 - y + 4 * half] if ny == 4 else [lax.rem(y + d, ny) for d in range(1, ny)]
    xpeers = [lax.rem(x + 2, nx), 3 - x, x + 1 - 2 * lax.rem(x, 2)] if nx == 4 else [lax.rem(x + d, nx) for d in range(1, nx)]

    def load_qkv(l):
        pairs = [(wq_hbm.at[l], wq), (wk_hbm.at[l], wk), (wv_hbm.at[l], wv)]
        return [pltpu.make_async_copy(s, d, wsem.at[l, i]) for i, (s, d) in enumerate(pairs)]

    def load_rest(l):
        out = [(k_hbm.at[l], kbuf.at[l]), (rel_hbm.at[l], rel.at[l]), (v_hbm.at[l], vbuf.at[l]), (wo_hbm.at[l], wo.at[l])]
        for c in range(ny):
            out.append((wup_hbm.at[l, :, pl.ds(c * ffc, ffc)], wup.at[l, c]))
        for c in range(ny):
            out.append((wdn_hbm.at[l, pl.ds(c * ffc, ffc), :], wdn.at[l, c]))
        return [pltpu.make_async_copy(s, d, wsem.at[l, 3 + i]) for i, (s, d) in enumerate(out)]

    for c in load_qkv(0):
        c.start()
    for l in range(layers):
        for c in load_rest(l):
            c.start()

    barrier = pltpu.get_barrier_semaphore()
    for py in ypeers:
        pl.semaphore_signal(barrier, inc=1, device_id=(r, py, x), device_id_type=MESH)
    for px in xpeers:
        pl.semaphore_signal(barrier, inc=1, device_id=(r, y, px), device_id_type=MESH)

    def iota(shape, dim):
        return lax.broadcasted_iota(jnp.int32, shape, dim)

    def ones_where(mask):
        return jnp.where(mask, 1.0, 0.0).astype(BF16)

    expand[...] = ones_where(iota((128, wide), 1) // heads == iota((128, wide), 0))

    def pick(s, shape, dim):
        j = iota(shape, dim)
        return (j // sloc) * rloc + s * sloc + j % sloc == iota(shape, 1 - dim)

    for s in range(ns):
        xcur[s] = dot(ones_where(pick(s, (srow, rows), 0)), x_ref[...]).astype(BF16)
    mi = iota((ny * grp, srow), 0)
    repeat = ones_where((mi // grp) * sloc + mi % sloc == iota((ny * grp, srow), 1))
    own_head = (iota((ny * grp, wide), 0) // sloc) % heads == iota((ny * grp, wide), 1) % heads
    irow = iota((srow, 128), 0)
    lrow = iota((srow, 128), 1)
    igrp = iota((grp, 128), 0) % sloc + sloc * y
    lgrp = iota((grp, 128), 1)

    pl.semaphore_wait(barrier, (ny - 1) + (nx - 1))

    def copy_y(l, s, ph, src, dst, py):
        return pltpu.make_async_remote_copy(
            src_ref=src, dst_ref=dst, send_sem=send_sem.at[l, s, ph, py], recv_sem=recv_sem.at[l, s, ph, y],
            device_id=(r, py, x), device_id_type=MESH)

    def copy_x(l, s, ph, src, dst, px):
        return pltpu.make_async_remote_copy(
            src_ref=src, dst_ref=dst, send_sem=send_sem.at[l, s, ph, px], recv_sem=recv_sem.at[l, s, ph, x],
            device_id=(r, y, px), device_id_type=MESH)

    def local(l, s, ph, buf, i):
        return pltpu.make_async_remote_copy(
            src_ref=buf, dst_ref=buf, send_sem=send_sem.at[l, s, ph, i], recv_sem=recv_sem.at[l, s, ph, i],
            device_id=(r, y, x), device_id_type=MESH)

    def gain_row(ref, l):
        g = ref[...].astype(F32)
        row = g[0:1]
        for i in range(1, layers):
            row = jnp.where(l == i, g[i:i + 1], row)
        return row

    def norm_local(l, s, ph, gain):
        xw = xcur[s].astype(F32)
        t = jnp.sum(xw * xw, axis=1, keepdims=True) * (1.0 / dm) + EPS
        t_row = jnp.sum(jnp.where(irow == lrow, jnp.broadcast_to(t, (srow, 128)), 0.0), axis=0, keepdims=True)
        stat[l, s, ph, y] = jnp.broadcast_to(t_row, (8, 128))
        for py in ypeers:
            copy_y(l, s, ph, stat.at[l, s, ph, y], stat.at[l, s, ph, y], py).start()
        return (xw * lax.rsqrt(t) * gain).astype(BF16)

    def ratio_rows(l, s, ph):
        for py in ypeers:
            local(l, s, ph, stat.at[l, s, ph, py], py).wait_recv()
        ts = [stat[l, s, ph, p][0:1] for p in range(ny)]
        mean = ts[0]
        for p in range(1, ny):
            mean = mean + ts[p]
        inv = lax.rsqrt(mean * (1.0 / ny))
        return [jnp.sqrt(t) * inv for t in ts]

    def reduce_start(l, s, ph, slot):
        for px in xpeers:
            copy_x(l, s, ph, ar.at[l, s, slot, x], ar.at[l, s, slot, x], px).start()

    def reduce_finish(l, s, ph, slot):
        for px in xpeers:
            local(l, s, ph, ar.at[l, s, slot, px], px).wait_recv()
        total = ar[l, s, slot, 0].astype(F32)
        for p in range(1, nx):
            total = total + ar[l, s, slot, p].astype(F32)
        xcur[s] = (xcur[s].astype(F32) + total).astype(BF16)

    PQ, PC, PA, PD, PU, PG = 2, 5, 6, 7, 8, 9

    def project(l, s, first):
        wl = load_qkv(l)
        h = norm_local(l, s, 0, gain_row(ga_ref, l))
        hrep[...] = dot(repeat, h).astype(BF16)
        for b in range(nblk):
            hx = dot(hrep[:, b * 128:(b + 1) * 128], expand[...])
            lhs[:, b * wide:(b + 1) * wide] = jnp.where(own_head, hx if b < nblk // 2 else -hx, 0.0).astype(BF16)
        kh = dm * heads // 2

        def scatter(i, part):
            for p in range(ny):
                qkv_send[s, i, p] = part[p * grp:(p + 1) * grp, :].astype(BF16)
            for py in ypeers:
                copy_y(l, s, PQ + i, qkv_send.at[s, i, py], qkv_recv.at[l, s, i, y], py).start()
            qkv_recv[l, s, i, y] = qkv_send[s, i, y]

        if first:
            wl[0].wait()
            wl[1].wait()
        qk = (dot(lhs[:, :kh], jnp.concatenate([wq[:kh, :], wk[:kh, :]], axis=1))
              - dot(lhs[:, kh:], jnp.concatenate([wq[kh:, :], wk[kh:, :]], axis=1)))
        scatter(0, qk[:, :hd])
        scatter(1, qk[:, hd:])
        if first:
            wl[2].wait()
        scatter(2, dot(lhs[:, :kh], wv[:kh, :]) - dot(lhs[:, kh:], wv[kh:, :]))

    sub = iota((heads, seq * heads), 0)
    col = iota((heads, seq * heads), 1)
    scale = hd ** -0.5

    def attend(l, s, first):
        wl = load_rest(l)
        own = (col % heads) == sub
        pos = col // heads
        ratios = ratio_rows(l, s, 0)
        cols = [jnp.sum(jnp.where(lgrp == igrp, ra, 0.0), axis=1, keepdims=True) for ra in ratios]

        def gather(i):
            for py in ypeers:
                local(l, s, PQ + i, qkv_recv.at[l, s, i, py], py).wait_recv()
            tot = qkv_recv[l, s, i, 0].astype(F32) * cols[0]
            for p in range(1, ny):
                tot = tot + qkv_recv[l, s, i, p].astype(F32) * cols[p]
            qkvf[i] = tot.astype(BF16).astype(F32)

        if first:
            wl[0].wait()
        gather(0)
        ul = u_ref[l].astype(F32)
        pl_bias = w_ref[l].astype(F32)
        rel0 = relrev[seq - 1].astype(F32)
        queries = []
        scores = []
        for b in range(sloc):
            length = len_ref[rloc * y + s * sloc + b]
            q = qkvf[0, pl.ds(b, heads, stride=sloc), :]
            a, cc = (q + ul).astype(BF16), (q + pl_bias).astype(BF16)
            queries.append((a, cc))
            window = relrev[pl.ds(seq - 1 - length, seq)].reshape(seq * heads, hd)
            sc = lax.dot_general(a, kbuf[l, s * sloc + b], NT, preferred_element_type=F32)
            sc = sc + lax.dot_general(cc, window, NT, preferred_element_type=F32)
            scores.append(jnp.where(own & (pos < length), sc * scale, -1e30))
        gather(1)
        if first:
            wl[2].wait()
        gather(2)
        for b in range(sloc):
            a, cc = queries[b]
            sc = scores[b]
            k = qkvf[1, pl.ds(b, heads, stride=sloc), :]
            v = qkvf[2, pl.ds(b, heads, stride=sloc), :]
            knew_ref[l, s * sloc + b] = k.astype(BF16)
            vnew_ref[l, s * sloc + b] = v.astype(BF16)
            sn = jnp.sum(a.astype(F32) * k + cc.astype(F32) * rel0, axis=1, keepdims=True) * scale
            m = jnp.maximum(jnp.max(sc, axis=1, keepdims=True), sn)
            e = jnp.exp(sc - m)
            en = jnp.exp(sn - m)
            z = jnp.sum(e, axis=1, keepdims=True) + en
            pr = (e / z).astype(BF16)
            pn = (en / z).astype(BF16).astype(F32)
            ctxf[b * heads:(b + 1) * heads, :] = dot(pr, vbuf[l, s * sloc + b]) + pn * v
        ctx_recv[l, s, y] = ctxf[0:grp, :].astype(BF16)
        for py in ypeers:
            copy_y(l, s, PC, ctx_recv.at[l, s, y], ctx_recv.at[l, s, y], py).start()

    def project_out(l, s, first):
        for py in ypeers:
            local(l, s, PC, ctx_recv.at[l, s, py], py).wait_recv()
        for p in range(ny):
            ctxf[p * grp:(p + 1) * grp, :] = ctx_recv[l, s, p].astype(F32)
        for j in range(heads):
            lhs_wo[:, j * hd:(j + 1) * hd] = ctxf[pl.ds(j, srow, stride=heads), :].astype(BF16)
        if first:
            load_rest(l)[3].wait()
        ar[l, s, 0, x] = dot(lhs_wo[...], wo[l]).astype(BF16)
        reduce_start(l, s, PA, 0)

    def ff_up(l, s, first):
        reduce_finish(l, s, PA, 0)
        h2 = norm_local(l, s, 1, gain_row(gm_ref, l))
        if first:
            for c in load_rest(l)[4:4 + ny]:
                c.wait()
        for py in ypeers:
            up_send[s, py] = dot(h2, wup[l, py]).astype(BF16)
            copy_y(l, s, PU, up_send.at[s, py], up_recv.at[l, s, y], py).start()
        up_recv[l, s, y] = dot(h2, wup[l, y]).astype(BF16)

    def ff_act(l, s, first):
        ratios = ratio_rows(l, s, 1)
        cols = [jnp.sum(jnp.where(lrow == irow, ra, 0.0), axis=1, keepdims=True) for ra in ratios]
        for py in ypeers:
            local(l, s, PU, up_recv.at[l, s, py], py).wait_recv()
        up = up_recv[l, s, 0].astype(F32) * cols[0]
        for p in range(1, ny):
            up = up + up_recv[l, s, p].astype(F32) * cols[p]
        up = up.astype(BF16).astype(F32)
        act[l, s, y] = jax.nn.gelu(up, approximate=True).astype(BF16)
        for py in ypeers:
            copy_y(l, s, PG, act.at[l, s, y], act.at[l, s, y], py).start()
        if first:
            for c in load_rest(l)[4 + ny:]:
                c.wait()
        down[s] = dot(act[l, s, y], wdn[l, y])

    def ff_down(l, s, first):
        for py in ypeers[::-1]:
            local(l, s, PG, act.at[l, s, py], py).wait_recv()
            down[s] += dot(act[l, s, py], wdn[l, py])
        ar[l, s, 1, x] = down[s].astype(BF16)
        reduce_start(l, s, PD, 1)

    def reverse_rel(l):
        load_rest(l)[1].wait()

        def rev(t, c):
            relrev[seq - 1 - t] = rel[l, t]
            return c

        lax.fori_loop(0, seq, rev, 0, unroll=8)

    relrev[pl.ds(seq, seq)] = jnp.zeros((seq, heads, hd), BF16)

    def layer(l, carry):
        for s in range(ns):
            @pl.when(l > 0)
            def _():
                reduce_finish(l - 1, s, PD, 1)

            project(l, s, s == 0)

        @pl.when(l + 1 < layers)
        def _():
            for c in load_qkv(l + 1):
                c.start()

        reverse_rel(l)
        for stage in (attend, project_out, ff_up, ff_act, ff_down):
            for s in range(ns):
                stage(l, s, s == 0)
        for s in range(ns):
            for py in ypeers:
                for i in range(3):
                    local(l, s, PQ + i, qkv_send.at[s, i, py], py).wait_send()
                local(l, s, PU, up_send.at[s, py], py).wait_send()
        return carry

    lax.fori_loop(0, layers, layer, 0)
    total = None
    for s in range(ns):
        reduce_finish(layers - 1, s, PD, 1)
        part = dot(ones_where(pick(s, (rows, srow), 1)), xcur[s])
        total = part if total is None else total + part
    xout_ref[...] = total.astype(BF16)

    def drain(l, carry):
        for s in range(ns):
            for py in ypeers:
                local(l, s, 0, stat.at[l, s, 0, y], py).wait_send()
                local(l, s, 1, stat.at[l, s, 1, y], py).wait_send()
                local(l, s, PC, ctx_recv.at[l, s, y], py).wait_send()
                local(l, s, PG, act.at[l, s, y], py).wait_send()
            for px in xpeers:
                local(l, s, PA, ar.at[l, s, 0, x], px).wait_send()
                local(l, s, PD, ar.at[l, s, 1, x], px).wait_send()
        return carry

    lax.fori_loop(0, layers, drain, 0)


def write_kernel(x_ref, len_ref, kn_ref, vn_ref, k_hbm, v_hbm, xout_ref, kout, vout, buf, in_sem, out_sem):
    layers, rloc = kn_ref.shape[:2]
    y = lax.axis_index("y")
    units = [(s, n, o, l) for l in range(layers) for s, n, o in ((k_hbm, kn_ref, kout), (v_hbm, vn_ref, vout))]
    nsplit = 2
    per = rloc // nsplit
    steps = [(s, n, o, l, q) for (s, n, o, l) in units for q in range(nsplit)]
    ins = [pltpu.make_async_copy(s.at[l, q * per:(q + 1) * per], buf.at[i], in_sem.at[i]) for i, (s, n, o, l, q) in enumerate(steps)]
    outs = [pltpu.make_async_copy(buf.at[i], o.at[l, q * per:(q + 1) * per], out_sem.at[i]) for i, (s, n, o, l, q) in enumerate(steps)]
    for c in ins:
        c.start()
    xout_ref[...] = x_ref[...]
    for i, (s, n, o, l, q) in enumerate(steps):
        ins[i].wait()
        for b in range(per):
            buf[i, b, len_ref[rloc * y + q * per + b]] = n[l, q * per + b]
        outs[i].start()
    for c in outs:
        c.wait()


def solution(mesh):
    ny, nx = mesh.shape["y"], mesh.shape["x"]
    cache_spec = P(None, ("rep", "y"), None, "x", None)
    row_spec = P("rep", "y")
    proj_spec = P(None, "y", "x", None)
    head_spec = P(None, "x", None)
    in_specs = (row_spec, P("rep"), cache_spec, cache_spec, P(None, None, "x", None), P(None, "y"),
                proj_spec, proj_spec, proj_spec, head_spec, head_spec, P(None, "x", None, "y"),
                P(None, "y"), P(None, "y", "x"), P(None, "x", "y"))
    out_specs = (row_spec, cache_spec, cache_spec)

    def local_step(hidden, lengths, k_cache, v_cache, rel_table, norm_attn, w_q, w_k, w_v, bias_content, bias_pos, w_out, norm_mlp, w_up, w_down):
        rows, dm = hidden.shape
        layers, rloc, seq, heads, hd = k_cache.shape
        ff = w_up.shape[2]
        ffc = ff // ny
        flat = (layers, dm * heads, hd)
        vm = pl.BlockSpec(memory_space=pltpu.VMEM)
        sm = pl.BlockSpec(memory_space=pltpu.SMEM)
        hbm = pl.BlockSpec(memory_space=pl.ANY)
        new_shape = jax.ShapeDtypeStruct((layers, rloc, heads, hd), BF16)
        ns = 2
        srow = rows // ns
        grp = heads * (rloc // ns)
        nph = 10
        npeer = max(ny, nx)
        out, k_new, v_new = pl.pallas_call(
            functools.partial(layers_kernel, ny, nx, ns),
            name="decode_layers",
            out_shape=(jax.ShapeDtypeStruct((rows, dm), BF16), new_shape, new_shape),
            in_specs=[vm, sm, hbm, hbm, hbm, vm, hbm, hbm, hbm, vm, vm, hbm, vm, hbm, hbm],
            out_specs=(vm, vm, vm),
            scratch_shapes=[
                pltpu.VMEM(flat[1:], BF16), pltpu.VMEM(flat[1:], BF16), pltpu.VMEM(flat[1:], BF16),
                pltpu.VMEM((layers, heads * hd, dm), BF16),
                pltpu.VMEM((layers, ny, dm, ffc), BF16),
                pltpu.VMEM((layers, ny, ffc, dm), BF16),
                pltpu.VMEM((layers, rloc, seq * heads, hd), BF16),
                pltpu.VMEM((layers, rloc, seq * heads, hd), BF16),
                pltpu.VMEM((layers, seq, heads, hd), BF16),
                pltpu.VMEM((2 * seq, heads, hd), BF16),
                pltpu.VMEM((ns, srow, dm), BF16),
                pltpu.VMEM((ny * grp, dm), BF16),
                pltpu.VMEM((128, 128 * heads), BF16),
                pltpu.VMEM((ny * grp, dm * heads), BF16),
                pltpu.VMEM((ns, 3, ny, grp, hd), BF16),
                pltpu.VMEM((layers, ns, 3, ny, grp, hd), BF16),
                pltpu.VMEM((layers, ns, 2, ny, 8, 128), F32),
                pltpu.VMEM((3, grp, hd), F32),
                pltpu.VMEM((ny * grp, hd), F32),
                pltpu.VMEM((layers, ns, ny, grp, hd), BF16),
                pltpu.VMEM((srow, heads * hd), BF16),
                pltpu.VMEM((layers, ns, 2, nx, srow, dm), BF16),
                pltpu.VMEM((ns, ny, srow, ffc), BF16),
                pltpu.VMEM((layers, ns, ny, srow, ffc), BF16),
                pltpu.VMEM((layers, ns, ny, srow, ffc), BF16),
                pltpu.VMEM((ns, srow, dm), F32),
                pltpu.SemaphoreType.DMA((layers, 7 + 2 * ny)),
                pltpu.SemaphoreType.DMA((layers, ns, nph, npeer)),
                pltpu.SemaphoreType.DMA((layers, ns, nph, npeer)),
            ],
            compiler_params=pltpu.CompilerParams(
                collective_id=0, has_side_effects=True, vmem_limit_bytes=67043328),
        )(hidden, lengths, k_cache.reshape(layers, rloc, seq * heads, hd), v_cache.reshape(layers, rloc, seq * heads, hd),
          rel_table, norm_attn, w_q.reshape(flat), w_k.reshape(flat), w_v.reshape(flat), bias_content, bias_pos,
          w_out.reshape(layers, heads * hd, dm), norm_mlp, w_up, w_down)
        nunit = 2 * layers * 2
        cache_shape = jax.ShapeDtypeStruct(k_cache.shape, BF16)
        return pl.pallas_call(
            write_kernel,
            name="write_caches",
            out_shape=(jax.ShapeDtypeStruct((rows, dm), BF16), cache_shape, cache_shape),
            in_specs=[vm, sm, vm, vm, hbm, hbm],
            out_specs=(vm, hbm, hbm),
            scratch_shapes=[
                pltpu.VMEM((nunit, rloc // 2, seq, heads, hd), BF16),
                pltpu.SemaphoreType.DMA((nunit,)),
                pltpu.SemaphoreType.DMA((nunit,)),
            ],
            compiler_params=pltpu.CompilerParams(vmem_limit_bytes=67043328),
        )(out, lengths, k_new, v_new, k_cache, v_cache)

    return jax.shard_map(local_step, mesh=mesh, in_specs=in_specs, out_specs=out_specs, check_vma=False)
```

```python
import functools

import jax
import jax.numpy as jnp
from jax import lax
from jax.experimental import pallas as pl
from jax.experimental.pallas import tpu as pltpu
from jax.sharding import PartitionSpec as P

EPS = 1e-6
MESH = pl.DeviceIdType.MESH
BF16 = jnp.bfloat16
F32 = jnp.float32
NT = (((1,), (1,)), ((), ()))


def dot(a, b):
    return jnp.dot(a, b, preferred_element_type=F32)


def layers_kernel(
    ny, nx, ns,
    x_hbm, len_hbm, k_hbm, v_hbm, rel_hbm, ga_hbm, wq_hbm, wk_hbm, wv_hbm, u_hbm, w_hbm, wo_hbm, gm_hbm, wup_hbm, wdn_hbm,
    out_ref,
    wq, wk, wv, wo, wup, wdn, kbuf, vbuf, rel, relrev,
    x_ref, len_ref, ga_ref, u_ref, w_ref, gm_ref,
    xcur, hrep, expand, lhs, qkv_send, qkv_recv, stat, qkvf, ctxf, ctx_recv, lhs_wo, ar, up_send, up_recv, act, down,
    ssem, wsem, send_sem, recv_sem,
):
    layers = wup_hbm.shape[0]
    rows, dm = x_ref.shape
    rloc = rows // ny
    srow = rows // ns
    sloc = rloc // ns
    heads, hd = u_ref.shape[1:]
    ffc = wup.shape[3]
    seq = rel_hbm.shape[1]
    nblk = dm // 128
    wide = 128 * heads
    grp = heads * sloc
    nxt = nblk * rows // 8
    r = lax.axis_index("rep")
    y = lax.axis_index("y")
    x = lax.axis_index("x")
    half = y // 2
    ypeers = [3 - 3 * half, 2 - half, 1 - y + 4 * half] if ny == 4 else [lax.rem(y + d, ny) for d in range(1, ny)]
    xpeers = [lax.rem(x + 2, nx), 3 - x, x + 1 - 2 * lax.rem(x, 2)] if nx == 4 else [lax.rem(x + d, nx) for d in range(1, nx)]

    def load_qkv(l):
        pairs = [(wq_hbm.at[l], wq), (wk_hbm.at[l], wk), (wv_hbm.at[l], wv)]
        return [pltpu.make_async_copy(s, d, wsem.at[l, i]) for i, (s, d) in enumerate(pairs)]

    def load_rest(l):
        out = [(k_hbm.at[l], kbuf), (rel_hbm.at[l], rel.at[l]), (v_hbm.at[l], vbuf), (wo_hbm.at[l], wo.at[l])]
        for c in range(ny):
            out.append((wup_hbm.at[l, :, pl.ds(c * ffc, ffc)], wup.at[l, c]))
        for c in range(ny):
            out.append((wdn_hbm.at[l, pl.ds(c * ffc, ffc), :], wdn.at[l, c]))
        return [pltpu.make_async_copy(s, d, wsem.at[l, 3 + i]) for i, (s, d) in enumerate(out)]

    smalls = [pltpu.make_async_copy(a, b, ssem.at[i]) for i, (a, b) in enumerate(
        ((x_hbm, x_ref), (ga_hbm, ga_ref), (len_hbm, len_ref), (u_hbm, u_ref), (w_hbm, w_ref), (gm_hbm, gm_ref)))]
    for c in smalls[:2] + load_qkv(0) + smalls[2:] + load_rest(0):
        c.start()
    for l in range(1, layers):
        rest = load_rest(l)
        for c in rest[1:2] + rest[3:]:
            c.start()

    barrier = pltpu.get_barrier_semaphore()
    for py in ypeers:
        pl.semaphore_signal(barrier, inc=1, device_id=(r, py, x), device_id_type=MESH)
    for px in xpeers:
        pl.semaphore_signal(barrier, inc=1, device_id=(r, y, px), device_id_type=MESH)

    for c in smalls:
        c.wait()

    def iota(shape, dim):
        return lax.broadcasted_iota(jnp.int32, shape, dim)

    def ones_where(mask):
        return jnp.where(mask, 1.0, 0.0).astype(BF16)

    expand[...] = ones_where(iota((128, wide), 1) // heads == iota((128, wide), 0))

    def pick(s, shape, dim):
        j = iota(shape, dim)
        return (j // sloc) * rloc + s * sloc + j % sloc == iota(shape, 1 - dim)

    for s in range(ns):
        xcur[s] = dot(ones_where(pick(s, (srow, rows), 0)), x_ref[...]).astype(BF16)
    mi = iota((ny * grp, srow), 0)
    repeat = ones_where((mi // grp) * sloc + mi % sloc == iota((ny * grp, srow), 1))
    own_head = (iota((ny * grp, wide), 0) // sloc) % heads == iota((ny * grp, wide), 1) % heads
    irow = iota((srow, 128), 0)
    lrow = iota((srow, 128), 1)
    igrp = iota((grp, 128), 0) % sloc + sloc * y
    lgrp = iota((grp, 128), 1)

    def copy_y(l, s, ph, src, dst, py):
        return pltpu.make_async_remote_copy(
            src_ref=src, dst_ref=dst, send_sem=send_sem.at[l, s, ph, py], recv_sem=recv_sem.at[l, s, ph, y],
            device_id=(r, py, x), device_id_type=MESH)

    def copy_x(l, s, ph, src, dst, px):
        return pltpu.make_async_remote_copy(
            src_ref=src, dst_ref=dst, send_sem=send_sem.at[l, s, ph, px], recv_sem=recv_sem.at[l, s, ph, x],
            device_id=(r, y, px), device_id_type=MESH)

    def local(l, s, ph, buf, i):
        return pltpu.make_async_remote_copy(
            src_ref=buf, dst_ref=buf, send_sem=send_sem.at[l, s, ph, i], recv_sem=recv_sem.at[l, s, ph, i],
            device_id=(r, y, x), device_id_type=MESH)

    def gain_row(ref, l):
        g = ref[...].astype(F32)
        row = g[0:1]
        for i in range(1, layers):
            row = jnp.where(l == i, g[i:i + 1], row)
        return row

    def norm_local(l, s, ph, gain):
        xw = xcur[s].astype(F32)
        t = jnp.sum(xw * xw, axis=1, keepdims=True) * (1.0 / dm) + EPS
        t_row = jnp.sum(jnp.where(irow == lrow, jnp.broadcast_to(t, (srow, 128)), 0.0), axis=0, keepdims=True)
        stat[l, s, ph, y] = jnp.broadcast_to(t_row, (8, 128))
        return (xw * lax.rsqrt(t) * gain).astype(BF16)

    def stat_send(l, s, ph):
        for py in ypeers:
            copy_y(l, s, ph, stat.at[l, s, ph, y], stat.at[l, s, ph, y], py).start()

    def ratio_rows(l, s, ph):
        for py in ypeers:
            local(l, s, ph, stat.at[l, s, ph, py], py).wait_recv()
        ts = [stat[l, s, ph, p][0:1] for p in range(ny)]
        mean = ts[0]
        for p in range(1, ny):
            mean = mean + ts[p]
        inv = lax.rsqrt(mean * (1.0 / ny))
        return [jnp.sqrt(t) * inv for t in ts]

    def reduce_start(l, s, ph, slot):
        for px in xpeers:
            copy_x(l, s, ph, ar.at[l, s, slot, x], ar.at[l, s, slot, x], px).start()

    def reduce_finish(l, s, ph, slot):
        for px in xpeers:
            local(l, s, ph, ar.at[l, s, slot, px], px).wait_recv()
        total = ar[l, s, slot, 0].astype(F32)
        for p in range(1, nx):
            total = total + ar[l, s, slot, p].astype(F32)
        xcur[s] = (xcur[s].astype(F32) + total).astype(BF16)

    PQ, PC, PA, PD, PU, PG = 2, 5, 6, 7, 8, 9

    kh = dm * heads // 2
    kq = kh // 2
    bh = nblk // 2
    mg = ny * grp

    def project(l, s, first, wait_barrier=False):
        wl = load_qkv(l)
        h = norm_local(l, s, 0, gain_row(ga_ref, l))
        if not wait_barrier:
            stat_send(l, s, 0)
        hrep[...] = dot(repeat, h).astype(BF16)
        for b in range(nblk):
            hx = dot(hrep[:, b * 128:(b + 1) * 128], expand[...])
            r0, c0 = (b // bh) * mg, (b % bh) * wide
            lhs[r0:r0 + mg, c0:c0 + wide] = jnp.where(own_head, hx if b < bh else -hx, 0.0).astype(BF16)

        def put(i, part):
            for p in range(ny):
                qkv_send[s, i, p] = part[p * grp:(p + 1) * grp, :].astype(BF16)

        def scatter(i):
            for py in ypeers:
                copy_y(l, s, PQ + i, qkv_send.at[s, i, py], qkv_recv.at[l, s, i, y], py).start()
            qkv_recv[l, s, i, y] = qkv_send[s, i, y]

        if first:
            wl[0].wait()
            wl[1].wait()
        qk = (dot(lhs[:mg, :], jnp.concatenate([wq[:kh, :], wk[:kh, :]], axis=1))
              - dot(lhs[mg:, :], jnp.concatenate([wq[kh:, :], wk[kh:, :]], axis=1)))
        put(0, qk[:, :hd])
        put(1, qk[:, hd:])
        if wait_barrier:
            pl.semaphore_wait(barrier, (ny - 1) + (nx - 1))
            stat_send(l, s, 0)
        scatter(0)
        scatter(1)
        if first:
            wl[2].wait()
        v1 = dot(lhs[:, :kq], jnp.concatenate([wv[:kq, :], wv[kh:kh + kq, :]], axis=1))
        v2 = dot(lhs[:, kq:], jnp.concatenate([wv[kq:kh, :], wv[kh + kq:, :]], axis=1))
        put(2, (v1[:mg, :hd] - v1[mg:, hd:]) + (v2[:mg, :hd] - v2[mg:, hd:]))
        scatter(2)

    sub = iota((heads, seq * heads), 0)
    col = iota((heads, seq * heads), 1)
    scale = hd ** -0.5

    def attend(l, s, first):
        wl = load_rest(l)
        own = (col % heads) == sub
        pos = col // heads
        ratios = ratio_rows(l, s, 0)
        cols = [jnp.sum(jnp.where(lgrp == igrp, ra, 0.0), axis=1, keepdims=True) for ra in ratios]

        def gather(i):
            for py in ypeers:
                local(l, s, PQ + i, qkv_recv.at[l, s, i, py], py).wait_recv()
            tot = qkv_recv[l, s, i, 0].astype(F32) * cols[0]
            for p in range(1, ny):
                tot = tot + qkv_recv[l, s, i, p].astype(F32) * cols[p]
            qkvf[i] = tot.astype(BF16).astype(F32)

        if first:
            wl[0].wait()
        gather(0)
        ul = u_ref[l].astype(F32)
        pl_bias = w_ref[l].astype(F32)
        rel0 = relrev[seq - 1].astype(F32)
        queries = []
        scores = []
        for b in range(sloc):
            length = len_ref[rloc * y + s * sloc + b]
            q = qkvf[0, pl.ds(b, heads, stride=sloc), :]
            a, cc = (q + ul).astype(BF16), (q + pl_bias).astype(BF16)
            queries.append((a, cc))
            window = relrev[pl.ds(seq - 1 - length, seq)].reshape(seq * heads, hd)
            sc = lax.dot_general(a, kbuf[s * sloc + b], NT, preferred_element_type=F32)
            sc = sc + lax.dot_general(cc, window, NT, preferred_element_type=F32)
            scores.append(jnp.where(own & (pos < length), sc * scale, -1e30))
        gather(1)
        if first:
            wl[2].wait()
        gather(2)
        for b in range(sloc):
            a, cc = queries[b]
            sc = scores[b]
            k = qkvf[1, pl.ds(b, heads, stride=sloc), :]
            v = qkvf[2, pl.ds(b, heads, stride=sloc), :]
            out_ref[nxt + l * rloc + s * sloc + b] = k.astype(BF16)
            out_ref[nxt + (layers + l) * rloc + s * sloc + b] = v.astype(BF16)
            sn = jnp.sum(a.astype(F32) * k + cc.astype(F32) * rel0, axis=1, keepdims=True) * scale
            m = jnp.maximum(jnp.max(sc, axis=1, keepdims=True), sn)
            e = jnp.exp(sc - m)
            en = jnp.exp(sn - m)
            z = jnp.sum(e, axis=1, keepdims=True) + en
            pr = (e / z).astype(BF16)
            pn = (en / z).astype(BF16).astype(F32)
            ctxf[b * heads:(b + 1) * heads, :] = dot(pr, vbuf[s * sloc + b]) + pn * v
        ctx_recv[l, s, y] = ctxf[0:grp, :].astype(BF16)
        for py in ypeers:
            copy_y(l, s, PC, ctx_recv.at[l, s, y], ctx_recv.at[l, s, y], py).start()

    def project_out(l, s, first):
        for py in ypeers:
            local(l, s, PC, ctx_recv.at[l, s, py], py).wait_recv()
        for p in range(ny):
            ctxf[p * grp:(p + 1) * grp, :] = ctx_recv[l, s, p].astype(F32)
        for j in range(heads):
            lhs_wo[:, j * hd:(j + 1) * hd] = ctxf[pl.ds(j, srow, stride=heads), :].astype(BF16)
        if first:
            load_rest(l)[3].wait()
        ar[l, s, 0, x] = dot(lhs_wo[...], wo[l]).astype(BF16)
        reduce_start(l, s, PA, 0)

    def ff_up(l, s, first):
        reduce_finish(l, s, PA, 0)
        h2 = norm_local(l, s, 1, gain_row(gm_ref, l))
        stat_send(l, s, 1)
        if first:
            for c in load_rest(l)[4:4 + ny]:
                c.wait()
        for py in ypeers:
            up_send[s, py] = dot(h2, wup[l, py]).astype(BF16)
            copy_y(l, s, PU, up_send.at[s, py], up_recv.at[l, s, y], py).start()
        up_recv[l, s, y] = dot(h2, wup[l, y]).astype(BF16)

    def ff_act(l, s, first):
        ratios = ratio_rows(l, s, 1)
        cols = [jnp.sum(jnp.where(lrow == irow, ra, 0.0), axis=1, keepdims=True) for ra in ratios]
        for py in ypeers:
            local(l, s, PU, up_recv.at[l, s, py], py).wait_recv()
        up = up_recv[l, s, 0].astype(F32) * cols[0]
        for p in range(1, ny):
            up = up + up_recv[l, s, p].astype(F32) * cols[p]
        up = up.astype(BF16).astype(F32)
        act[l, s, y] = jax.nn.gelu(up, approximate=True).astype(BF16)
        for py in ypeers:
            copy_y(l, s, PG, act.at[l, s, y], act.at[l, s, y], py).start()
        if first:
            for c in load_rest(l)[4 + ny:]:
                c.wait()
        down[s] = dot(act[l, s, y], wdn[l, y])

    def ff_down(l, s, first):
        for py in ypeers[::-1]:
            local(l, s, PG, act.at[l, s, py], py).wait_recv()
            down[s] += dot(act[l, s, py], wdn[l, py])
        ar[l, s, 1, x] = down[s].astype(BF16)
        reduce_start(l, s, PD, 1)

    def reverse_rel(l):
        load_rest(l)[1].wait()

        def rev(t, c):
            relrev[seq - 1 - t] = rel[l, t]
            return c

        lax.fori_loop(0, seq, rev, 0, unroll=8)

    relrev[pl.ds(seq, seq)] = jnp.zeros((seq, heads, hd), BF16)

    for s in range(ns):
        project(0, s, s == 0, wait_barrier=s == 0)

    def layer(l, carry):
        @pl.when(l + 1 < layers)
        def _():
            for c in load_qkv(l + 1):
                c.start()

        reverse_rel(l)
        for s in range(ns):
            attend(l, s, s == 0)

        @pl.when(l + 1 < layers)
        def _():
            rest = load_rest(l + 1)
            rest[0].start()
            rest[2].start()

        for stage in (project_out, ff_up, ff_act, ff_down):
            for s in range(ns):
                stage(l, s, s == 0)
        for s in range(ns):
            for py in ypeers:
                for i in range(3):
                    local(l, s, PQ + i, qkv_send.at[s, i, py], py).wait_send()
                local(l, s, PU, up_send.at[s, py], py).wait_send()

        @pl.when(l + 1 < layers)
        def _():
            for s in range(ns):
                reduce_finish(l, s, PD, 1)
                project(l + 1, s, s == 0)

        return carry

    lax.fori_loop(0, layers, layer, 0)
    total = None
    for s in range(ns):
        reduce_finish(layers - 1, s, PD, 1)
        part = dot(ones_where(pick(s, (rows, srow), 1)), xcur[s])
        total = part if total is None else total + part
    for j in range(nblk):
        out_ref[j * rows // 8:(j + 1) * rows // 8] = total[:, j * 128:(j + 1) * 128].astype(BF16).reshape(rows // 8, 8, 128)

    def drain(l, carry):
        for s in range(ns):
            for py in ypeers:
                local(l, s, 0, stat.at[l, s, 0, y], py).wait_send()
                local(l, s, 1, stat.at[l, s, 1, y], py).wait_send()
                local(l, s, PC, ctx_recv.at[l, s, y], py).wait_send()
                local(l, s, PG, act.at[l, s, y], py).wait_send()
            for px in xpeers:
                local(l, s, PA, ar.at[l, s, 0, x], px).wait_send()
                local(l, s, PD, ar.at[l, s, 1, x], px).wait_send()
        return carry

    lax.fori_loop(0, layers, drain, 0)


def write_kernel(len_ref, new_hbm, k_ref, v_ref, xout_hbm, kout, vout, x_buf, new_ref, small_sem, bulk_sem, row_sem):
    layers, rloc = k_ref.shape[:2]
    rows, dm = x_buf.shape
    nblk = dm // 128
    y = lax.axis_index("y")
    units = [(i, src, out, l, b) for l in range(layers) for i, (src, out) in enumerate(((k_ref, kout), (v_ref, vout))) for b in range(rloc)]
    bulk = [pltpu.make_async_copy(src.at[l, b], out.at[l, b], bulk_sem.at[n]) for n, (i, src, out, l, b) in enumerate(units)]
    late = [pltpu.make_async_copy(new_ref.at[nblk * rows // 8 + (i * layers + l) * rloc + b], out.at[l, b, len_ref[rloc * y + b]], row_sem.at[n])
            for n, (i, src, out, l, b) in enumerate(units)]
    news = pltpu.make_async_copy(new_hbm, new_ref, small_sem.at[0])
    news.start()
    for c in bulk:
        c.start()
    news.wait()
    for j in range(nblk):
        x_buf[:, j * 128:(j + 1) * 128] = new_ref[j * rows // 8:(j + 1) * rows // 8].reshape(rows, 128)
    xout = pltpu.make_async_copy(x_buf, xout_hbm, small_sem.at[1])
    xout.start()
    for c, n in zip(bulk, late):
        c.wait()
        n.start()
    for n in late:
        n.wait()
    xout.wait()


def solution(mesh):
    ny, nx = mesh.shape["y"], mesh.shape["x"]
    cache_spec = P(None, ("rep", "y"), None, "x", None)
    row_spec = P("rep", "y")
    proj_spec = P(None, "y", "x", None)
    head_spec = P(None, "x", None)
    in_specs = (row_spec, P("rep"), cache_spec, cache_spec, P(None, None, "x", None), P(None, "y"),
                proj_spec, proj_spec, proj_spec, head_spec, head_spec, P(None, "x", None, "y"),
                P(None, "y"), P(None, "y", "x"), P(None, "x", "y"))
    out_specs = (row_spec, cache_spec, cache_spec)

    def local_step(hidden, lengths, k_cache, v_cache, rel_table, norm_attn, w_q, w_k, w_v, bias_content, bias_pos, w_out, norm_mlp, w_up, w_down):
        rows, dm = hidden.shape
        layers, rloc, seq, heads, hd = k_cache.shape
        ff = w_up.shape[2]
        ffc = ff // ny
        flat = (layers, dm * heads, hd)
        vm = pl.BlockSpec(memory_space=pltpu.VMEM)
        sm = pl.BlockSpec(memory_space=pltpu.SMEM)
        hbm = pl.BlockSpec(memory_space=pl.ANY)
        hbm_only = pl.BlockSpec(memory_space=pltpu.HBM)
        new_shape = jax.ShapeDtypeStruct((dm // 128 * rows // 8 + 2 * layers * rloc, 8, 128), BF16)
        ns = 2
        srow = rows // ns
        grp = heads * (rloc // ns)
        nph = 10
        npeer = max(ny, nx)
        out = pl.pallas_call(
            functools.partial(layers_kernel, ny, nx, ns),
            name="decode_layers",
            out_shape=new_shape,
            in_specs=[hbm] * 15,
            out_specs=vm,
            scratch_shapes=[
                pltpu.VMEM(flat[1:], BF16), pltpu.VMEM(flat[1:], BF16), pltpu.VMEM(flat[1:], BF16),
                pltpu.VMEM((layers, heads * hd, dm), BF16),
                pltpu.VMEM((layers, ny, dm, ffc), BF16),
                pltpu.VMEM((layers, ny, ffc, dm), BF16),
                pltpu.VMEM((rloc, seq * heads, hd), BF16),
                pltpu.VMEM((rloc, seq * heads, hd), BF16),
                pltpu.VMEM((layers, seq, heads, hd), BF16),
                pltpu.VMEM((2 * seq, heads, hd), BF16),
                pltpu.VMEM((rows, dm), BF16), pltpu.SMEM(lengths.shape, jnp.int32), pltpu.VMEM(norm_attn.shape, BF16),
                pltpu.VMEM(bias_content.shape, BF16), pltpu.VMEM(bias_pos.shape, BF16), pltpu.VMEM(norm_mlp.shape, BF16),
                pltpu.VMEM((ns, srow, dm), BF16),
                pltpu.VMEM((ny * grp, dm), BF16),
                pltpu.VMEM((128, 128 * heads), BF16),
                pltpu.VMEM((2 * ny * grp, dm * heads // 2), BF16),
                pltpu.VMEM((ns, 3, ny, grp, hd), BF16),
                pltpu.VMEM((layers, ns, 3, ny, grp, hd), BF16),
                pltpu.VMEM((layers, ns, 2, ny, 8, 128), F32),
                pltpu.VMEM((3, grp, hd), F32),
                pltpu.VMEM((ny * grp, hd), F32),
                pltpu.VMEM((layers, ns, ny, grp, hd), BF16),
                pltpu.VMEM((srow, heads * hd), BF16),
                pltpu.VMEM((layers, ns, 2, nx, srow, dm), BF16),
                pltpu.VMEM((ns, ny, srow, ffc), BF16),
                pltpu.VMEM((layers, ns, ny, srow, ffc), BF16),
                pltpu.VMEM((layers, ns, ny, srow, ffc), BF16),
                pltpu.VMEM((ns, srow, dm), F32),
                pltpu.SemaphoreType.DMA((6,)),
                pltpu.SemaphoreType.DMA((layers, 7 + 2 * ny)),
                pltpu.SemaphoreType.DMA((layers, ns, nph, npeer)),
                pltpu.SemaphoreType.DMA((layers, ns, nph, npeer)),
            ],
            compiler_params=pltpu.CompilerParams(
                collective_id=0, has_side_effects=True, vmem_limit_bytes=109 << 19),
        )(hidden, lengths, k_cache.reshape(layers, rloc, seq * heads, hd), v_cache.reshape(layers, rloc, seq * heads, hd),
          rel_table, norm_attn, w_q.reshape(flat), w_k.reshape(flat), w_v.reshape(flat), bias_content, bias_pos,
          w_out.reshape(layers, heads * hd, dm), norm_mlp, w_up, w_down)
        nunit = 2 * layers * rloc
        cache_shape = jax.ShapeDtypeStruct(k_cache.shape, BF16)
        return pl.pallas_call(
            write_kernel,
            name="write_caches",
            out_shape=(jax.ShapeDtypeStruct((rows, dm), BF16), cache_shape, cache_shape),
            in_specs=[sm, hbm_only, vm, vm],
            out_specs=(hbm, hbm, hbm),
            scratch_shapes=[
                pltpu.VMEM((rows, dm), BF16), pltpu.VMEM(new_shape.shape, BF16),
                pltpu.SemaphoreType.DMA((2,)), pltpu.SemaphoreType.DMA((nunit,)), pltpu.SemaphoreType.DMA((nunit,)),
            ],
            compiler_params=pltpu.CompilerParams(vmem_limit_bytes=16777216),
        )(lengths, out, k_cache, v_cache)

    return jax.shard_map(local_step, mesh=mesh, in_specs=in_specs, out_specs=out_specs, check_vma=False)
```

```python
import functools

import jax
import jax.numpy as jnp
from jax import lax
from jax.experimental import pallas as pl
from jax.experimental.pallas import tpu as pltpu
from jax.sharding import PartitionSpec as P

EPS = 1e-6
MESH = pl.DeviceIdType.MESH
BF16 = jnp.bfloat16
F32 = jnp.float32
NT = (((1,), (1,)), ((), ()))


def dot(a, b):
    return jnp.dot(a, b, preferred_element_type=F32)


def layers_kernel(
    ny, nx, ns,
    x_ref, len_ref, k_hbm, v_hbm, rel_hbm, ga_ref, wq_hbm, wk_hbm, wv_hbm, u_ref, w_ref, wo_hbm, gm_ref, wup_hbm, wdn_hbm,
    out_ref,
    wq, wk, wv, wo, wup, wdn, kbuf, vbuf, rel, relrev,
    xcur, hrep, expand, lhs, qkv_send, qkv_recv, stat, qkvf, ctxf, ctx_recv, lhs_wo, ar, up_send, up_recv, act, down,
    wsem, send_sem, recv_sem,
):
    layers = wup_hbm.shape[0]
    rows, dm = x_ref.shape
    rloc = rows // ny
    srow = rows // ns
    sloc = rloc // ns
    heads, hd = u_ref.shape[1:]
    ffc = wup.shape[3]
    seq = rel_hbm.shape[1]
    nblk = dm // 128
    wide = 128 * heads
    grp = heads * sloc
    nxt = nblk * rows // 8
    r = lax.axis_index("rep")
    y = lax.axis_index("y")
    x = lax.axis_index("x")
    half = y // 2
    ypeers = [3 - 3 * half, 2 - half, 1 - y + 4 * half] if ny == 4 else [lax.rem(y + d, ny) for d in range(1, ny)]
    xpeers = [lax.rem(x + 2, nx), 3 - x, x + 1 - 2 * lax.rem(x, 2)] if nx == 4 else [lax.rem(x + d, nx) for d in range(1, nx)]

    def load_qkv(l):
        pairs = [(wq_hbm.at[l], wq), (wk_hbm.at[l], wk), (wv_hbm.at[l], wv)]
        return [pltpu.make_async_copy(s, d, wsem.at[l, i]) for i, (s, d) in enumerate(pairs)]

    def load_rest(l):
        out = [(k_hbm.at[l], kbuf.at[l]), (rel_hbm.at[l], rel.at[l]), (v_hbm.at[l], vbuf.at[l]), (wo_hbm.at[l], wo.at[l])]
        for c in range(ny):
            out.append((wup_hbm.at[l, :, pl.ds(c * ffc, ffc)], wup.at[l, c]))
        for c in range(ny):
            out.append((wdn_hbm.at[l, pl.ds(c * ffc, ffc), :], wdn.at[l, c]))
        return [pltpu.make_async_copy(s, d, wsem.at[l, 3 + i]) for i, (s, d) in enumerate(out)]

    for c in load_qkv(0):
        c.start()
    for l in range(layers):
        for c in load_rest(l):
            c.start()

    barrier = pltpu.get_barrier_semaphore()
    for py in ypeers:
        pl.semaphore_signal(barrier, inc=1, device_id=(r, py, x), device_id_type=MESH)
    for px in xpeers:
        pl.semaphore_signal(barrier, inc=1, device_id=(r, y, px), device_id_type=MESH)

    def iota(shape, dim):
        return lax.broadcasted_iota(jnp.int32, shape, dim)

    def ones_where(mask):
        return jnp.where(mask, 1.0, 0.0).astype(BF16)

    expand[...] = ones_where(iota((128, wide), 1) // heads == iota((128, wide), 0))

    def pick(s, shape, dim):
        j = iota(shape, dim)
        return (j // sloc) * rloc + s * sloc + j % sloc == iota(shape, 1 - dim)

    for s in range(ns):
        xcur[s] = dot(ones_where(pick(s, (srow, rows), 0)), x_ref[...]).astype(BF16)
    mi = iota((ny * grp, srow), 0)
    repeat = ones_where((mi // grp) * sloc + mi % sloc == iota((ny * grp, srow), 1))
    own_head = (iota((ny * grp, wide), 0) // sloc) % heads == iota((ny * grp, wide), 1) % heads
    irow = iota((srow, 128), 0)
    lrow = iota((srow, 128), 1)
    igrp = iota((grp, 128), 0) % sloc + sloc * y
    lgrp = iota((grp, 128), 1)

    pl.semaphore_wait(barrier, (ny - 1) + (nx - 1))

    def copy_y(l, s, ph, src, dst, py):
        return pltpu.make_async_remote_copy(
            src_ref=src, dst_ref=dst, send_sem=send_sem.at[l, s, ph, py], recv_sem=recv_sem.at[l, s, ph, y],
            device_id=(r, py, x), device_id_type=MESH)

    def copy_x(l, s, ph, src, dst, px):
        return pltpu.make_async_remote_copy(
            src_ref=src, dst_ref=dst, send_sem=send_sem.at[l, s, ph, px], recv_sem=recv_sem.at[l, s, ph, x],
            device_id=(r, y, px), device_id_type=MESH)

    def local(l, s, ph, buf, i):
        return pltpu.make_async_remote_copy(
            src_ref=buf, dst_ref=buf, send_sem=send_sem.at[l, s, ph, i], recv_sem=recv_sem.at[l, s, ph, i],
            device_id=(r, y, x), device_id_type=MESH)

    def gain_row(ref, l):
        g = ref[...].astype(F32)
        row = g[0:1]
        for i in range(1, layers):
            row = jnp.where(l == i, g[i:i + 1], row)
        return row

    def norm_local(l, s, ph, gain):
        xw = xcur[s].astype(F32)
        t = jnp.sum(xw * xw, axis=1, keepdims=True) * (1.0 / dm) + EPS
        t_row = jnp.sum(jnp.where(irow == lrow, jnp.broadcast_to(t, (srow, 128)), 0.0), axis=0, keepdims=True)
        stat[l, s, ph, y] = jnp.broadcast_to(t_row, (8, 128))
        for py in ypeers:
            copy_y(l, s, ph, stat.at[l, s, ph, y], stat.at[l, s, ph, y], py).start()
        return (xw * lax.rsqrt(t) * gain).astype(BF16)

    def ratio_rows(l, s, ph):
        for py in ypeers:
            local(l, s, ph, stat.at[l, s, ph, py], py).wait_recv()
        ts = [stat[l, s, ph, p][0:1] for p in range(ny)]
        mean = ts[0]
        for p in range(1, ny):
            mean = mean + ts[p]
        inv = lax.rsqrt(mean * (1.0 / ny))
        return [jnp.sqrt(t) * inv for t in ts]

    def reduce_start(l, s, ph, slot):
        for px in xpeers:
            copy_x(l, s, ph, ar.at[l, s, slot, x], ar.at[l, s, slot, x], px).start()

    def reduce_finish(l, s, ph, slot):
        for px in xpeers:
            local(l, s, ph, ar.at[l, s, slot, px], px).wait_recv()
        total = ar[l, s, slot, 0].astype(F32)
        for p in range(1, nx):
            total = total + ar[l, s, slot, p].astype(F32)
        xcur[s] = (xcur[s].astype(F32) + total).astype(BF16)

    PQ, PC, PA, PD, PU, PG = 2, 5, 6, 7, 8, 9

    kh = dm * heads // 2
    kq = kh // 2
    bh = nblk // 2
    mg = ny * grp

    def project(l, s, first):
        wl = load_qkv(l)
        h = norm_local(l, s, 0, gain_row(ga_ref, l))
        hrep[...] = dot(repeat, h).astype(BF16)
        for b in range(nblk):
            hx = dot(hrep[:, b * 128:(b + 1) * 128], expand[...])
            r0, c0 = (b // bh) * mg, (b % bh) * wide
            lhs[r0:r0 + mg, c0:c0 + wide] = jnp.where(own_head, hx if b < bh else -hx, 0.0).astype(BF16)

        def put(i, part):
            for p in range(ny):
                qkv_send[s, i, p] = part[p * grp:(p + 1) * grp, :].astype(BF16)

        def scatter(i):
            for py in ypeers:
                copy_y(l, s, PQ + i, qkv_send.at[s, i, py], qkv_recv.at[l, s, i, y], py).start()
            qkv_recv[l, s, i, y] = qkv_send[s, i, y]

        if first:
            wl[0].wait()
            wl[1].wait()
        qk = (dot(lhs[:mg, :], jnp.concatenate([wq[:kh, :], wk[:kh, :]], axis=1))
              - dot(lhs[mg:, :], jnp.concatenate([wq[kh:, :], wk[kh:, :]], axis=1)))
        put(0, qk[:, :hd])
        put(1, qk[:, hd:])
        scatter(0)
        scatter(1)
        if first:
            wl[2].wait()
        v1 = dot(lhs[:, :kq], jnp.concatenate([wv[:kq, :], wv[kh:kh + kq, :]], axis=1))
        v2 = dot(lhs[:, kq:], jnp.concatenate([wv[kq:kh, :], wv[kh + kq:, :]], axis=1))
        put(2, (v1[:mg, :hd] - v1[mg:, hd:]) + (v2[:mg, :hd] - v2[mg:, hd:]))
        scatter(2)

    sub = iota((heads, seq * heads), 0)
    col = iota((heads, seq * heads), 1)
    scale = hd ** -0.5

    def attend(l, s, first):
        wl = load_rest(l)
        own = (col % heads) == sub
        pos = col // heads
        ratios = ratio_rows(l, s, 0)
        cols = [jnp.sum(jnp.where(lgrp == igrp, ra, 0.0), axis=1, keepdims=True) for ra in ratios]

        def gather(i):
            for py in ypeers:
                local(l, s, PQ + i, qkv_recv.at[l, s, i, py], py).wait_recv()
            tot = qkv_recv[l, s, i, 0].astype(F32) * cols[0]
            for p in range(1, ny):
                tot = tot + qkv_recv[l, s, i, p].astype(F32) * cols[p]
            qkvf[i] = tot.astype(BF16).astype(F32)

        if first:
            wl[0].wait()
        gather(0)
        ul = u_ref[l].astype(F32)
        pl_bias = w_ref[l].astype(F32)
        rel0 = relrev[seq - 1].astype(F32)
        queries = []
        scores = []
        for b in range(sloc):
            length = len_ref[rloc * y + s * sloc + b]
            q = qkvf[0, pl.ds(b, heads, stride=sloc), :]
            a, cc = (q + ul).astype(BF16), (q + pl_bias).astype(BF16)
            queries.append((a, cc))
            window = relrev[pl.ds(seq - 1 - length, seq)].reshape(seq * heads, hd)
            sc = lax.dot_general(a, kbuf[l, s * sloc + b], NT, preferred_element_type=F32)
            sc = sc + lax.dot_general(cc, window, NT, preferred_element_type=F32)
            scores.append(jnp.where(own & (pos < length), sc * scale, -1e30))
        gather(1)
        if first:
            wl[2].wait()
        gather(2)
        for b in range(sloc):
            a, cc = queries[b]
            sc = scores[b]
            k = qkvf[1, pl.ds(b, heads, stride=sloc), :]
            v = qkvf[2, pl.ds(b, heads, stride=sloc), :]
            out_ref[nxt + l * rloc + s * sloc + b] = k.astype(BF16)
            out_ref[nxt + (layers + l) * rloc + s * sloc + b] = v.astype(BF16)
            sn = jnp.sum(a.astype(F32) * k + cc.astype(F32) * rel0, axis=1, keepdims=True) * scale
            m = jnp.maximum(jnp.max(sc, axis=1, keepdims=True), sn)
            e = jnp.exp(sc - m)
            en = jnp.exp(sn - m)
            z = jnp.sum(e, axis=1, keepdims=True) + en
            pr = (e / z).astype(BF16)
            pn = (en / z).astype(BF16).astype(F32)
            ctxf[b * heads:(b + 1) * heads, :] = dot(pr, vbuf[l, s * sloc + b]) + pn * v
        ctx_recv[l, s, y] = ctxf[0:grp, :].astype(BF16)
        for py in ypeers:
            copy_y(l, s, PC, ctx_recv.at[l, s, y], ctx_recv.at[l, s, y], py).start()

    def project_out(l, s, first):
        for py in ypeers:
            local(l, s, PC, ctx_recv.at[l, s, py], py).wait_recv()
        for p in range(ny):
            ctxf[p * grp:(p + 1) * grp, :] = ctx_recv[l, s, p].astype(F32)
        for j in range(heads):
            lhs_wo[:, j * hd:(j + 1) * hd] = ctxf[pl.ds(j, srow, stride=heads), :].astype(BF16)
        if first:
            load_rest(l)[3].wait()
        ar[l, s, 0, x] = dot(lhs_wo[...], wo[l]).astype(BF16)
        reduce_start(l, s, PA, 0)

    def ff_up(l, s, first):
        reduce_finish(l, s, PA, 0)
        h2 = norm_local(l, s, 1, gain_row(gm_ref, l))
        if first:
            for c in load_rest(l)[4:4 + ny]:
                c.wait()
        for py in ypeers:
            up_send[s, py] = dot(h2, wup[l, py]).astype(BF16)
            copy_y(l, s, PU, up_send.at[s, py], up_recv.at[l, s, y], py).start()
        up_recv[l, s, y] = dot(h2, wup[l, y]).astype(BF16)

    def ff_act(l, s, first):
        ratios = ratio_rows(l, s, 1)
        cols = [jnp.sum(jnp.where(lrow == irow, ra, 0.0), axis=1, keepdims=True) for ra in ratios]
        for py in ypeers:
            local(l, s, PU, up_recv.at[l, s, py], py).wait_recv()
        up = up_recv[l, s, 0].astype(F32) * cols[0]
        for p in range(1, ny):
            up = up + up_recv[l, s, p].astype(F32) * cols[p]
        up = up.astype(BF16).astype(F32)
        act[l, s, y] = jax.nn.gelu(up, approximate=True).astype(BF16)
        for py in ypeers:
            copy_y(l, s, PG, act.at[l, s, y], act.at[l, s, y], py).start()
        if first:
            for c in load_rest(l)[4 + ny:]:
                c.wait()
        down[s] = dot(act[l, s, y], wdn[l, y])

    def ff_down(l, s, first):
        for py in ypeers[::-1]:
            local(l, s, PG, act.at[l, s, py], py).wait_recv()
            down[s] += dot(act[l, s, py], wdn[l, py])
        ar[l, s, 1, x] = down[s].astype(BF16)
        reduce_start(l, s, PD, 1)

    def reverse_rel(l):
        load_rest(l)[1].wait()

        def rev(t, c):
            relrev[seq - 1 - t] = rel[l, t]
            return c

        lax.fori_loop(0, seq, rev, 0, unroll=8)

    relrev[pl.ds(seq, seq)] = jnp.zeros((seq, heads, hd), BF16)

    def layer(l, carry):
        for s in range(ns):
            @pl.when(l > 0)
            def _():
                reduce_finish(l - 1, s, PD, 1)

            project(l, s, s == 0)

        @pl.when(l + 1 < layers)
        def _():
            for c in load_qkv(l + 1):
                c.start()

        reverse_rel(l)
        for stage in (attend, project_out, ff_up, ff_act, ff_down):
            for s in range(ns):
                stage(l, s, s == 0)
        for s in range(ns):
            for py in ypeers:
                for i in range(3):
                    local(l, s, PQ + i, qkv_send.at[s, i, py], py).wait_send()
                local(l, s, PU, up_send.at[s, py], py).wait_send()
        return carry

    lax.fori_loop(0, layers, layer, 0)
    total = None
    for s in range(ns):
        reduce_finish(layers - 1, s, PD, 1)
        part = dot(ones_where(pick(s, (rows, srow), 1)), xcur[s])
        total = part if total is None else total + part
    for j in range(nblk):
        out_ref[j * rows // 8:(j + 1) * rows // 8] = total[:, j * 128:(j + 1) * 128].astype(BF16).reshape(rows // 8, 8, 128)

    def drain(l, carry):
        for s in range(ns):
            for py in ypeers:
                local(l, s, 0, stat.at[l, s, 0, y], py).wait_send()
                local(l, s, 1, stat.at[l, s, 1, y], py).wait_send()
                local(l, s, PC, ctx_recv.at[l, s, y], py).wait_send()
                local(l, s, PG, act.at[l, s, y], py).wait_send()
            for px in xpeers:
                local(l, s, PA, ar.at[l, s, 0, x], px).wait_send()
                local(l, s, PD, ar.at[l, s, 1, x], px).wait_send()
        return carry

    lax.fori_loop(0, layers, drain, 0)


def write_kernel(len_hbm, new_hbm, k_hbm, v_hbm, xout_hbm, kout, vout, len_ref, x_buf, new_ref, buf, small_sem, in_sem, out_sem):
    layers, rloc = k_hbm.shape[:2]
    rows, dm = x_buf.shape
    nblk = dm // 128
    per = buf.shape[1]
    y = lax.axis_index("y")
    units = [(i, src, out, l, q * per) for l in range(layers) for i, (src, out) in enumerate(((k_hbm, kout), (v_hbm, vout)))
             for q in range(rloc // per)]
    smalls = [pltpu.make_async_copy(len_hbm, len_ref, small_sem.at[0]), pltpu.make_async_copy(new_hbm, new_ref, small_sem.at[1])]
    ins = [pltpu.make_async_copy(src.at[l, pl.ds(q, per)], buf.at[n], in_sem.at[n]) for n, (i, src, out, l, q) in enumerate(units)]
    outs = [pltpu.make_async_copy(buf.at[n], out.at[l, pl.ds(q, per)], out_sem.at[n]) for n, (i, src, out, l, q) in enumerate(units)]
    for c in smalls + ins:
        c.start()
    for c in smalls:
        c.wait()
    for j in range(nblk):
        x_buf[:, j * 128:(j + 1) * 128] = new_ref[j * rows // 8:(j + 1) * rows // 8].reshape(rows, 128)
    xout = pltpu.make_async_copy(x_buf, xout_hbm, small_sem.at[2])
    xout.start()
    for n, (i, src, out, l, q) in enumerate(units):
        ins[n].wait()
        for b in range(per):
            buf[n, b, len_ref[rloc * y + q + b]] = new_ref[nblk * rows // 8 + (i * layers + l) * rloc + q + b]
        outs[n].start()
    for c in outs:
        c.wait()
    xout.wait()


def solution(mesh):
    ny, nx = mesh.shape["y"], mesh.shape["x"]
    cache_spec = P(None, ("rep", "y"), None, "x", None)
    row_spec = P("rep", "y")
    proj_spec = P(None, "y", "x", None)
    head_spec = P(None, "x", None)
    in_specs = (row_spec, P("rep"), cache_spec, cache_spec, P(None, None, "x", None), P(None, "y"),
                proj_spec, proj_spec, proj_spec, head_spec, head_spec, P(None, "x", None, "y"),
                P(None, "y"), P(None, "y", "x"), P(None, "x", "y"))
    out_specs = (row_spec, cache_spec, cache_spec)

    def local_step(hidden, lengths, k_cache, v_cache, rel_table, norm_attn, w_q, w_k, w_v, bias_content, bias_pos, w_out, norm_mlp, w_up, w_down):
        rows, dm = hidden.shape
        layers, rloc, seq, heads, hd = k_cache.shape
        ff = w_up.shape[2]
        ffc = ff // ny
        flat = (layers, dm * heads, hd)
        vm = pl.BlockSpec(memory_space=pltpu.VMEM)
        sm = pl.BlockSpec(memory_space=pltpu.SMEM)
        hbm = pl.BlockSpec(memory_space=pl.ANY)
        new_shape = jax.ShapeDtypeStruct((dm // 128 * rows // 8 + 2 * layers * rloc, 8, 128), BF16)
        ns = 2
        srow = rows // ns
        grp = heads * (rloc // ns)
        nph = 10
        npeer = max(ny, nx)
        out = pl.pallas_call(
            functools.partial(layers_kernel, ny, nx, ns),
            name="decode_layers",
            out_shape=new_shape,
            in_specs=[vm, sm, hbm, hbm, hbm, vm, hbm, hbm, hbm, vm, vm, hbm, vm, hbm, hbm],
            out_specs=vm,
            scratch_shapes=[
                pltpu.VMEM(flat[1:], BF16), pltpu.VMEM(flat[1:], BF16), pltpu.VMEM(flat[1:], BF16),
                pltpu.VMEM((layers, heads * hd, dm), BF16),
                pltpu.VMEM((layers, ny, dm, ffc), BF16),
                pltpu.VMEM((layers, ny, ffc, dm), BF16),
                pltpu.VMEM((layers, rloc, seq * heads, hd), BF16),
                pltpu.VMEM((layers, rloc, seq * heads, hd), BF16),
                pltpu.VMEM((layers, seq, heads, hd), BF16),
                pltpu.VMEM((2 * seq, heads, hd), BF16),
                pltpu.VMEM((ns, srow, dm), BF16),
                pltpu.VMEM((ny * grp, dm), BF16),
                pltpu.VMEM((128, 128 * heads), BF16),
                pltpu.VMEM((2 * ny * grp, dm * heads // 2), BF16),
                pltpu.VMEM((ns, 3, ny, grp, hd), BF16),
                pltpu.VMEM((layers, ns, 3, ny, grp, hd), BF16),
                pltpu.VMEM((layers, ns, 2, ny, 8, 128), F32),
                pltpu.VMEM((3, grp, hd), F32),
                pltpu.VMEM((ny * grp, hd), F32),
                pltpu.VMEM((layers, ns, ny, grp, hd), BF16),
                pltpu.VMEM((srow, heads * hd), BF16),
                pltpu.VMEM((layers, ns, 2, nx, srow, dm), BF16),
                pltpu.VMEM((ns, ny, srow, ffc), BF16),
                pltpu.VMEM((layers, ns, ny, srow, ffc), BF16),
                pltpu.VMEM((layers, ns, ny, srow, ffc), BF16),
                pltpu.VMEM((ns, srow, dm), F32),
                pltpu.SemaphoreType.DMA((layers, 7 + 2 * ny)),
                pltpu.SemaphoreType.DMA((layers, ns, nph, npeer)),
                pltpu.SemaphoreType.DMA((layers, ns, nph, npeer)),
            ],
            compiler_params=pltpu.CompilerParams(
                collective_id=0, has_side_effects=True, vmem_limit_bytes=67043328),
        )(hidden, lengths, k_cache.reshape(layers, rloc, seq * heads, hd), v_cache.reshape(layers, rloc, seq * heads, hd),
          rel_table, norm_attn, w_q.reshape(flat), w_k.reshape(flat), w_v.reshape(flat), bias_content, bias_pos,
          w_out.reshape(layers, heads * hd, dm), norm_mlp, w_up, w_down)
        per = 2
        nunit = 2 * layers * (rloc // per)
        cache_shape = jax.ShapeDtypeStruct(k_cache.shape, BF16)
        return pl.pallas_call(
            write_kernel,
            name="write_caches",
            out_shape=(jax.ShapeDtypeStruct((rows, dm), BF16), cache_shape, cache_shape),
            in_specs=[hbm] * 4,
            out_specs=(hbm, hbm, hbm),
            scratch_shapes=[
                pltpu.SMEM(lengths.shape, jnp.int32),
                pltpu.VMEM((rows, dm), BF16),
                pltpu.VMEM(new_shape.shape, BF16),
                pltpu.VMEM((nunit, per, seq, heads, hd), BF16),
                pltpu.SemaphoreType.DMA((3,)),
                pltpu.SemaphoreType.DMA((nunit,)),
                pltpu.SemaphoreType.DMA((nunit,)),
            ],
            compiler_params=pltpu.CompilerParams(vmem_limit_bytes=67043328),
        )(lengths, out, k_cache, v_cache)

    return jax.shard_map(local_step, mesh=mesh, in_specs=in_specs, out_specs=out_specs, check_vma=False)
```

```python
import functools

import jax
import jax.numpy as jnp
from jax import lax
from jax.experimental import pallas as pl
from jax.experimental.pallas import tpu as pltpu
from jax.sharding import PartitionSpec as P

EPS = 1e-6
MESH = pl.DeviceIdType.MESH
BF16 = jnp.bfloat16
F32 = jnp.float32
NT = (((1,), (1,)), ((), ()))


def dot(a, b):
    return jnp.dot(a, b, preferred_element_type=F32)


def layers_kernel(
    ny, nx, ns,
    x_ref, len_ref, k_hbm, v_hbm, rel_hbm, ga_ref, wq_hbm, wk_hbm, wv_hbm, u_ref, w_ref, wo_hbm, gm_ref, wup_hbm, wdn_hbm,
    out_ref,
    wq, wk, wv, wo, wup, wdn, kbuf, vbuf, rel, relrev,
    xcur, hrep, expand, lhs, qkv_send, qkv_recv, stat, qkvf, ctxf, ctx_recv, lhs_wo, ar, up_send, up_recv, act, down,
    wsem, send_sem, recv_sem,
):
    layers = wup_hbm.shape[0]
    rows, dm = x_ref.shape
    rloc = rows // ny
    srow = rows // ns
    sloc = rloc // ns
    heads, hd = u_ref.shape[1:]
    ffc = wup.shape[3]
    seq = rel_hbm.shape[1]
    nblk = dm // 128
    wide = 128 * heads
    grp = heads * sloc
    nxt = nblk * rows // 8
    r = lax.axis_index("rep")
    y = lax.axis_index("y")
    x = lax.axis_index("x")
    half = y // 2
    ypeers = [3 - 3 * half, 2 - half, 1 - y + 4 * half] if ny == 4 else [lax.rem(y + d, ny) for d in range(1, ny)]
    xpeers = [lax.rem(x + 2, nx), 3 - x, x + 1 - 2 * lax.rem(x, 2)] if nx == 4 else [lax.rem(x + d, nx) for d in range(1, nx)]

    def load_qkv(l):
        pairs = [(wq_hbm.at[l], wq), (wk_hbm.at[l], wk), (wv_hbm.at[l], wv)]
        return [pltpu.make_async_copy(s, d, wsem.at[l, i]) for i, (s, d) in enumerate(pairs)]

    def load_rest(l):
        out = [(k_hbm.at[l], kbuf.at[l]), (rel_hbm.at[l], rel.at[l]), (v_hbm.at[l], vbuf.at[l]), (wo_hbm.at[l], wo.at[l])]
        for c in range(ny):
            out.append((wup_hbm.at[l, :, pl.ds(c * ffc, ffc)], wup.at[l, c]))
        for c in range(ny):
            out.append((wdn_hbm.at[l, pl.ds(c * ffc, ffc), :], wdn.at[l, c]))
        return [pltpu.make_async_copy(s, d, wsem.at[l, 3 + i]) for i, (s, d) in enumerate(out)]

    for c in load_qkv(0):
        c.start()
    for l in range(layers):
        for c in load_rest(l):
            c.start()

    barrier = pltpu.get_barrier_semaphore()
    for py in ypeers:
        pl.semaphore_signal(barrier, inc=1, device_id=(r, py, x), device_id_type=MESH)
    for px in xpeers:
        pl.semaphore_signal(barrier, inc=1, device_id=(r, y, px), device_id_type=MESH)

    def iota(shape, dim):
        return lax.broadcasted_iota(jnp.int32, shape, dim)

    def ones_where(mask):
        return jnp.where(mask, 1.0, 0.0).astype(BF16)

    expand[...] = ones_where(iota((128, wide), 1) // heads == iota((128, wide), 0))

    def pick(s, shape, dim):
        j = iota(shape, dim)
        return (j // sloc) * rloc + s * sloc + j % sloc == iota(shape, 1 - dim)

    for s in range(ns):
        xcur[s] = dot(ones_where(pick(s, (srow, rows), 0)), x_ref[...]).astype(BF16)
    mi = iota((ny * grp, srow), 0)
    repeat = ones_where((mi // grp) * sloc + mi % sloc == iota((ny * grp, srow), 1))
    own_head = (iota((ny * grp, wide), 0) // sloc) % heads == iota((ny * grp, wide), 1) % heads
    irow = iota((srow, 128), 0)
    lrow = iota((srow, 128), 1)
    igrp = iota((grp, 128), 0) % sloc + sloc * y
    lgrp = iota((grp, 128), 1)

    def copy_y(l, s, ph, src, dst, py):
        return pltpu.make_async_remote_copy(
            src_ref=src, dst_ref=dst, send_sem=send_sem.at[l, s, ph, py], recv_sem=recv_sem.at[l, s, ph, y],
            device_id=(r, py, x), device_id_type=MESH)

    def copy_x(l, s, ph, src, dst, px):
        return pltpu.make_async_remote_copy(
            src_ref=src, dst_ref=dst, send_sem=send_sem.at[l, s, ph, px], recv_sem=recv_sem.at[l, s, ph, x],
            device_id=(r, y, px), device_id_type=MESH)

    def local(l, s, ph, buf, i):
        return pltpu.make_async_remote_copy(
            src_ref=buf, dst_ref=buf, send_sem=send_sem.at[l, s, ph, i], recv_sem=recv_sem.at[l, s, ph, i],
            device_id=(r, y, x), device_id_type=MESH)

    def gain_row(ref, l):
        g = ref[...].astype(F32)
        row = g[0:1]
        for i in range(1, layers):
            row = jnp.where(l == i, g[i:i + 1], row)
        return row

    def norm_local(l, s, ph, gain):
        xw = xcur[s].astype(F32)
        t = jnp.sum(xw * xw, axis=1, keepdims=True) * (1.0 / dm) + EPS
        t_row = jnp.sum(jnp.where(irow == lrow, jnp.broadcast_to(t, (srow, 128)), 0.0), axis=0, keepdims=True)
        stat[l, s, ph, y] = jnp.broadcast_to(t_row, (8, 128))
        return (xw * lax.rsqrt(t) * gain).astype(BF16)

    def stat_send(l, s, ph):
        for py in ypeers:
            copy_y(l, s, ph, stat.at[l, s, ph, y], stat.at[l, s, ph, y], py).start()

    def ratio_rows(l, s, ph):
        for py in ypeers:
            local(l, s, ph, stat.at[l, s, ph, py], py).wait_recv()
        ts = [stat[l, s, ph, p][0:1] for p in range(ny)]
        mean = ts[0]
        for p in range(1, ny):
            mean = mean + ts[p]
        inv = lax.rsqrt(mean * (1.0 / ny))
        return [jnp.sqrt(t) * inv for t in ts]

    def reduce_start(l, s, ph, slot):
        for px in xpeers:
            copy_x(l, s, ph, ar.at[l, s, slot, x], ar.at[l, s, slot, x], px).start()

    def reduce_finish(l, s, ph, slot):
        for px in xpeers:
            local(l, s, ph, ar.at[l, s, slot, px], px).wait_recv()
        total = ar[l, s, slot, 0].astype(F32)
        for p in range(1, nx):
            total = total + ar[l, s, slot, p].astype(F32)
        xcur[s] = (xcur[s].astype(F32) + total).astype(BF16)

    PQ, PC, PA, PD, PU, PG = 2, 5, 6, 7, 8, 9

    kh = dm * heads // 2
    kq = kh // 2
    bh = nblk // 2
    mg = ny * grp

    def project(l, s, first, wait_barrier=False):
        wl = load_qkv(l)
        h = norm_local(l, s, 0, gain_row(ga_ref, l))
        if not wait_barrier:
            stat_send(l, s, 0)
        hrep[...] = dot(repeat, h).astype(BF16)
        for b in range(nblk):
            hx = dot(hrep[:, b * 128:(b + 1) * 128], expand[...])
            r0, c0 = (b // bh) * mg, (b % bh) * wide
            lhs[r0:r0 + mg, c0:c0 + wide] = jnp.where(own_head, hx if b < bh else -hx, 0.0).astype(BF16)

        def put(i, part):
            for p in range(ny):
                qkv_send[s, i, p] = part[p * grp:(p + 1) * grp, :].astype(BF16)

        def scatter(i):
            for py in ypeers:
                copy_y(l, s, PQ + i, qkv_send.at[s, i, py], qkv_recv.at[l, s, i, y], py).start()
            qkv_recv[l, s, i, y] = qkv_send[s, i, y]

        if first:
            wl[0].wait()
            wl[1].wait()
        qk = (dot(lhs[:mg, :], jnp.concatenate([wq[:kh, :], wk[:kh, :]], axis=1))
              - dot(lhs[mg:, :], jnp.concatenate([wq[kh:, :], wk[kh:, :]], axis=1)))
        put(0, qk[:, :hd])
        put(1, qk[:, hd:])
        if wait_barrier:
            pl.semaphore_wait(barrier, (ny - 1) + (nx - 1))
            stat_send(l, s, 0)
        scatter(0)
        scatter(1)
        if first:
            wl[2].wait()
        v1 = dot(lhs[:, :kq], jnp.concatenate([wv[:kq, :], wv[kh:kh + kq, :]], axis=1))
        v2 = dot(lhs[:, kq:], jnp.concatenate([wv[kq:kh, :], wv[kh + kq:, :]], axis=1))
        put(2, (v1[:mg, :hd] - v1[mg:, hd:]) + (v2[:mg, :hd] - v2[mg:, hd:]))
        scatter(2)

    sub = iota((heads, seq * heads), 0)
    col = iota((heads, seq * heads), 1)
    scale = hd ** -0.5

    def attend(l, s, first):
        wl = load_rest(l)
        own = (col % heads) == sub
        pos = col // heads
        ratios = ratio_rows(l, s, 0)
        cols = [jnp.sum(jnp.where(lgrp == igrp, ra, 0.0), axis=1, keepdims=True) for ra in ratios]

        def gather(i):
            for py in ypeers:
                local(l, s, PQ + i, qkv_recv.at[l, s, i, py], py).wait_recv()
            tot = qkv_recv[l, s, i, 0].astype(F32) * cols[0]
            for p in range(1, ny):
                tot = tot + qkv_recv[l, s, i, p].astype(F32) * cols[p]
            qkvf[i] = tot.astype(BF16).astype(F32)

        if first:
            wl[0].wait()
        gather(0)
        ul = u_ref[l].astype(F32)
        pl_bias = w_ref[l].astype(F32)
        rel0 = relrev[seq - 1].astype(F32)
        queries = []
        scores = []
        for b in range(sloc):
            length = len_ref[rloc * y + s * sloc + b]
            q = qkvf[0, pl.ds(b, heads, stride=sloc), :]
            a, cc = (q + ul).astype(BF16), (q + pl_bias).astype(BF16)
            queries.append((a, cc))
            window = relrev[pl.ds(seq - 1 - length, seq)].reshape(seq * heads, hd)
            sc = lax.dot_general(a, kbuf[l, s * sloc + b], NT, preferred_element_type=F32)
            sc = sc + lax.dot_general(cc, window, NT, preferred_element_type=F32)
            scores.append(jnp.where(own & (pos < length), sc * scale, -1e30))
        gather(1)
        if first:
            wl[2].wait()
        gather(2)
        for b in range(sloc):
            a, cc = queries[b]
            sc = scores[b]
            k = qkvf[1, pl.ds(b, heads, stride=sloc), :]
            v = qkvf[2, pl.ds(b, heads, stride=sloc), :]
            out_ref[nxt + l * rloc + s * sloc + b] = k.astype(BF16)
            out_ref[nxt + (layers + l) * rloc + s * sloc + b] = v.astype(BF16)
            sn = jnp.sum(a.astype(F32) * k + cc.astype(F32) * rel0, axis=1, keepdims=True) * scale
            m = jnp.maximum(jnp.max(sc, axis=1, keepdims=True), sn)
            e = jnp.exp(sc - m)
            en = jnp.exp(sn - m)
            z = jnp.sum(e, axis=1, keepdims=True) + en
            pr = (e / z).astype(BF16)
            pn = (en / z).astype(BF16).astype(F32)
            ctxf[b * heads:(b + 1) * heads, :] = dot(pr, vbuf[l, s * sloc + b]) + pn * v
        ctx_recv[l, s, y] = ctxf[0:grp, :].astype(BF16)
        for py in ypeers:
            copy_y(l, s, PC, ctx_recv.at[l, s, y], ctx_recv.at[l, s, y], py).start()

    def project_out(l, s, first):
        for py in ypeers:
            local(l, s, PC, ctx_recv.at[l, s, py], py).wait_recv()
        for p in range(ny):
            ctxf[p * grp:(p + 1) * grp, :] = ctx_recv[l, s, p].astype(F32)
        for j in range(heads):
            lhs_wo[:, j * hd:(j + 1) * hd] = ctxf[pl.ds(j, srow, stride=heads), :].astype(BF16)
        if first:
            load_rest(l)[3].wait()
        ar[l, s, 0, x] = dot(lhs_wo[...], wo[l]).astype(BF16)
        reduce_start(l, s, PA, 0)

    def ff_up(l, s, first):
        reduce_finish(l, s, PA, 0)
        h2 = norm_local(l, s, 1, gain_row(gm_ref, l))
        stat_send(l, s, 1)
        if first:
            for c in load_rest(l)[4:4 + ny]:
                c.wait()
        for py in ypeers:
            up_send[s, py] = dot(h2, wup[l, py]).astype(BF16)
            copy_y(l, s, PU, up_send.at[s, py], up_recv.at[l, s, y], py).start()
        up_recv[l, s, y] = dot(h2, wup[l, y]).astype(BF16)

    def ff_act(l, s, first):
        ratios = ratio_rows(l, s, 1)
        cols = [jnp.sum(jnp.where(lrow == irow, ra, 0.0), axis=1, keepdims=True) for ra in ratios]
        for py in ypeers:
            local(l, s, PU, up_recv.at[l, s, py], py).wait_recv()
        up = up_recv[l, s, 0].astype(F32) * cols[0]
        for p in range(1, ny):
            up = up + up_recv[l, s, p].astype(F32) * cols[p]
        up = up.astype(BF16).astype(F32)
        act[l, s, y] = jax.nn.gelu(up, approximate=True).astype(BF16)
        for py in ypeers:
            copy_y(l, s, PG, act.at[l, s, y], act.at[l, s, y], py).start()
        if first:
            for c in load_rest(l)[4 + ny:]:
                c.wait()
        down[s] = dot(act[l, s, y], wdn[l, y])

    def ff_down(l, s, first):
        for py in ypeers[::-1]:
            local(l, s, PG, act.at[l, s, py], py).wait_recv()
            down[s] += dot(act[l, s, py], wdn[l, py])
        ar[l, s, 1, x] = down[s].astype(BF16)
        reduce_start(l, s, PD, 1)

    def reverse_rel(l):
        load_rest(l)[1].wait()

        def rev(t, c):
            relrev[seq - 1 - t] = rel[l, t]
            return c

        lax.fori_loop(0, seq, rev, 0, unroll=8)

    relrev[pl.ds(seq, seq)] = jnp.zeros((seq, heads, hd), BF16)

    for s in range(ns):
        project(0, s, s == 0, wait_barrier=s == 0)

    def layer(l, carry):
        @pl.when(l + 1 < layers)
        def _():
            for c in load_qkv(l + 1):
                c.start()

        reverse_rel(l)
        for s in range(ns):
            attend(l, s, s == 0)

        for stage in (project_out, ff_up, ff_act, ff_down):
            for s in range(ns):
                stage(l, s, s == 0)
        for s in range(ns):
            for py in ypeers:
                for i in range(3):
                    local(l, s, PQ + i, qkv_send.at[s, i, py], py).wait_send()
                local(l, s, PU, up_send.at[s, py], py).wait_send()

        @pl.when(l + 1 < layers)
        def _():
            for s in range(ns):
                reduce_finish(l, s, PD, 1)
                project(l + 1, s, s == 0)

        return carry

    lax.fori_loop(0, layers, layer, 0)
    total = None
    for s in range(ns):
        reduce_finish(layers - 1, s, PD, 1)
        part = dot(ones_where(pick(s, (rows, srow), 1)), xcur[s])
        total = part if total is None else total + part
    for j in range(nblk):
        out_ref[j * rows // 8:(j + 1) * rows // 8] = total[:, j * 128:(j + 1) * 128].astype(BF16).reshape(rows // 8, 8, 128)

    def drain(l, carry):
        for s in range(ns):
            for py in ypeers:
                local(l, s, 0, stat.at[l, s, 0, y], py).wait_send()
                local(l, s, 1, stat.at[l, s, 1, y], py).wait_send()
                local(l, s, PC, ctx_recv.at[l, s, y], py).wait_send()
                local(l, s, PG, act.at[l, s, y], py).wait_send()
            for px in xpeers:
                local(l, s, PA, ar.at[l, s, 0, x], px).wait_send()
                local(l, s, PD, ar.at[l, s, 1, x], px).wait_send()
        return carry

    lax.fori_loop(0, layers, drain, 0)


def write_kernel(len_hbm, new_hbm, k_hbm, v_hbm, xout_hbm, kout, vout, len_ref, x_buf, new_ref, buf, small_sem, in_sem, out_sem):
    layers, rloc = k_hbm.shape[:2]
    rows, dm = x_buf.shape
    nblk = dm // 128
    per = buf.shape[1]
    y = lax.axis_index("y")
    units = [(i, src, out, l, q * per) for l in range(layers) for i, (src, out) in enumerate(((k_hbm, kout), (v_hbm, vout)))
             for q in range(rloc // per)]
    smalls = [pltpu.make_async_copy(len_hbm, len_ref, small_sem.at[0]), pltpu.make_async_copy(new_hbm, new_ref, small_sem.at[1])]
    ins = [pltpu.make_async_copy(src.at[l, pl.ds(q, per)], buf.at[n], in_sem.at[n]) for n, (i, src, out, l, q) in enumerate(units)]
    outs = [pltpu.make_async_copy(buf.at[n], out.at[l, pl.ds(q, per)], out_sem.at[n]) for n, (i, src, out, l, q) in enumerate(units)]
    for c in smalls + ins:
        c.start()
    for c in smalls:
        c.wait()
    for j in range(nblk):
        x_buf[:, j * 128:(j + 1) * 128] = new_ref[j * rows // 8:(j + 1) * rows // 8].reshape(rows, 128)
    xout = pltpu.make_async_copy(x_buf, xout_hbm, small_sem.at[2])
    xout.start()
    for n, (i, src, out, l, q) in enumerate(units):
        ins[n].wait()
        for b in range(per):
            buf[n, b, len_ref[rloc * y + q + b]] = new_ref[nblk * rows // 8 + (i * layers + l) * rloc + q + b]
        outs[n].start()
    for c in outs:
        c.wait()
    xout.wait()


def solution(mesh):
    ny, nx = mesh.shape["y"], mesh.shape["x"]
    cache_spec = P(None, ("rep", "y"), None, "x", None)
    row_spec = P("rep", "y")
    proj_spec = P(None, "y", "x", None)
    head_spec = P(None, "x", None)
    in_specs = (row_spec, P("rep"), cache_spec, cache_spec, P(None, None, "x", None), P(None, "y"),
                proj_spec, proj_spec, proj_spec, head_spec, head_spec, P(None, "x", None, "y"),
                P(None, "y"), P(None, "y", "x"), P(None, "x", "y"))
    out_specs = (row_spec, cache_spec, cache_spec)

    def local_step(hidden, lengths, k_cache, v_cache, rel_table, norm_attn, w_q, w_k, w_v, bias_content, bias_pos, w_out, norm_mlp, w_up, w_down):
        rows, dm = hidden.shape
        layers, rloc, seq, heads, hd = k_cache.shape
        ff = w_up.shape[2]
        ffc = ff // ny
        flat = (layers, dm * heads, hd)
        vm = pl.BlockSpec(memory_space=pltpu.VMEM)
        sm = pl.BlockSpec(memory_space=pltpu.SMEM)
        hbm = pl.BlockSpec(memory_space=pl.ANY)
        new_shape = jax.ShapeDtypeStruct((dm // 128 * rows // 8 + 2 * layers * rloc, 8, 128), BF16)
        ns = 2
        srow = rows // ns
        grp = heads * (rloc // ns)
        nph = 10
        npeer = max(ny, nx)
        out = pl.pallas_call(
            functools.partial(layers_kernel, ny, nx, ns),
            name="decode_layers",
            out_shape=new_shape,
            in_specs=[vm, sm, hbm, hbm, hbm, vm, hbm, hbm, hbm, vm, vm, hbm, vm, hbm, hbm],
            out_specs=vm,
            scratch_shapes=[
                pltpu.VMEM(flat[1:], BF16), pltpu.VMEM(flat[1:], BF16), pltpu.VMEM(flat[1:], BF16),
                pltpu.VMEM((layers, heads * hd, dm), BF16),
                pltpu.VMEM((layers, ny, dm, ffc), BF16),
                pltpu.VMEM((layers, ny, ffc, dm), BF16),
                pltpu.VMEM((layers, rloc, seq * heads, hd), BF16),
                pltpu.VMEM((layers, rloc, seq * heads, hd), BF16),
                pltpu.VMEM((layers, seq, heads, hd), BF16),
                pltpu.VMEM((2 * seq, heads, hd), BF16),
                pltpu.VMEM((ns, srow, dm), BF16),
                pltpu.VMEM((ny * grp, dm), BF16),
                pltpu.VMEM((128, 128 * heads), BF16),
                pltpu.VMEM((2 * ny * grp, dm * heads // 2), BF16),
                pltpu.VMEM((ns, 3, ny, grp, hd), BF16),
                pltpu.VMEM((layers, ns, 3, ny, grp, hd), BF16),
                pltpu.VMEM((layers, ns, 2, ny, 8, 128), F32),
                pltpu.VMEM((3, grp, hd), F32),
                pltpu.VMEM((ny * grp, hd), F32),
                pltpu.VMEM((layers, ns, ny, grp, hd), BF16),
                pltpu.VMEM((srow, heads * hd), BF16),
                pltpu.VMEM((layers, ns, 2, nx, srow, dm), BF16),
                pltpu.VMEM((ns, ny, srow, ffc), BF16),
                pltpu.VMEM((layers, ns, ny, srow, ffc), BF16),
                pltpu.VMEM((layers, ns, ny, srow, ffc), BF16),
                pltpu.VMEM((ns, srow, dm), F32),
                pltpu.SemaphoreType.DMA((layers, 7 + 2 * ny)),
                pltpu.SemaphoreType.DMA((layers, ns, nph, npeer)),
                pltpu.SemaphoreType.DMA((layers, ns, nph, npeer)),
            ],
            compiler_params=pltpu.CompilerParams(
                collective_id=0, has_side_effects=True, vmem_limit_bytes=67043328),
        )(hidden, lengths, k_cache.reshape(layers, rloc, seq * heads, hd), v_cache.reshape(layers, rloc, seq * heads, hd),
          rel_table, norm_attn, w_q.reshape(flat), w_k.reshape(flat), w_v.reshape(flat), bias_content, bias_pos,
          w_out.reshape(layers, heads * hd, dm), norm_mlp, w_up, w_down)
        per = 2
        nunit = 2 * layers * (rloc // per)
        cache_shape = jax.ShapeDtypeStruct(k_cache.shape, BF16)
        return pl.pallas_call(
            write_kernel,
            name="write_caches",
            out_shape=(jax.ShapeDtypeStruct((rows, dm), BF16), cache_shape, cache_shape),
            in_specs=[hbm] * 4,
            out_specs=(hbm, hbm, hbm),
            scratch_shapes=[
                pltpu.SMEM(lengths.shape, jnp.int32),
                pltpu.VMEM((rows, dm), BF16),
                pltpu.VMEM(new_shape.shape, BF16),
                pltpu.VMEM((nunit, per, seq, heads, hd), BF16),
                pltpu.SemaphoreType.DMA((3,)),
                pltpu.SemaphoreType.DMA((nunit,)),
                pltpu.SemaphoreType.DMA((nunit,)),
            ],
            compiler_params=pltpu.CompilerParams(vmem_limit_bytes=67043328),
        )(lengths, out, k_cache, v_cache)

    return jax.shard_map(local_step, mesh=mesh, in_specs=in_specs, out_specs=out_specs, check_vma=False)
```
